256 devices in a mesh: node: 4 (over x), sx: 16 (over z_hi, y), sy: 4 (over z_lo, core).
Axes of the slice: x: 4, y: 4, z: 8 (z_hi: 4, z_lo: 2; z = z_hi * 2 + z_lo), core: 2. Of those that a mesh axis runs over, the one named last changes fastest.
Arguments:
- previous: float32 [4, 2, 256, 128, 256], P('node', None, 'sx', 'sy'), may hold values from 0 to 1
- feed_rate: float32 [256, 128, 256], P('sx', 'sy'), may hold values from 0.01 to 0.1
- kill_rate: float32 [256, 128, 256], P('sx', 'sy'), may hold values from 0.03 to 0.1
Outputs:
- sections: float32 [4, 2, 256, 128, 256], P('node', None, 'sx', 'sy')
The draws below stay inside these ranges and needn't reach their ends.
All inputs are finite; a program needn't handle non-finite values.
Results may differ from the reference program's by a relative error of at most 0.00011.
Values sent between devices are 32-bit elements; how exact they have to be, the bound alone decides.
No kernel may reach another device: no remote copies, remote signals or barrier semaphores. Data moves between devices by JAX's collectives and lax.ppermute only.
A program may use at most 64 MiB of HBM per device.

```python
import math
import jax
import jax.numpy as jnp
from jax import lax

M = 4
SPECIES = 2
SWEEPS = 2
JACOBI = 12
NZ = 256
NX = 256
NY = 128


def draw_previous(key, part):
    local_key = jax.random.fold_in(key, 7301)
    first_index = jnp.arange(NX, dtype=jnp.int32)[:, None, None]
    second_index = jnp.arange(NY, dtype=jnp.int32)[None, :, None]
    third_index = jnp.arange(NZ, dtype=jnp.int32)[None, None, :]
    parity = (first_index + second_index + third_index) % 2
    pattern = (1 - 2 * parity).astype(jnp.float32)
    uniform_part = jax.random.uniform(local_key, (M, SPECIES, NX, NY, NZ), jnp.float32)
    factor = 0.5 + 0.5 * uniform_part
    values = 0.5 + 0.49 * factor * pattern[None, None]
    return values.astype(jnp.float32)


def levels(key, dims, split, least, top_value):
    def one(axis_at, parts):
        heights = jax.random.uniform(jax.random.fold_in(jax.random.fold_in(key, 6), axis_at), (parts,), jnp.float32, least / len(split), top_value / len(split))
        return jnp.repeat(jnp.exp(heights), dims[axis_at] // parts).reshape((-1,) + (1,) * (len(dims) - axis_at - 1))

    loudness = one(*split[0])
    for cut in split[1:]:
        loudness = loudness * one(*cut)
    return loudness


def setup_inputs(seed: int = 0) -> dict:
    key_of = jax.random.split(jax.random.key(seed), 4)
    previous = draw_previous(jax.random.fold_in(key_of[3], 71), 0)
    feed_rate = jnp.clip(jnp.exp(math.log(0.1) - 2.3025851 * jax.random.uniform(key_of[1], (NX, NY, NZ), jnp.float32) ** levels(key_of[1], (NX, NY, NZ), ((0, 16), (1, 4)), -0.2, 0.2)), 0.01, 0.1)
    kill_rate = jnp.clip(jnp.exp(math.log(0.1) - 1.2039728 * jax.random.uniform(key_of[2], (NX, NY, NZ), jnp.float32) ** levels(key_of[2], (NX, NY, NZ), ((0, 16), (1, 4)), -0.2, 0.2)), 0.03, 0.1)
    return {"previous": previous, "feed_rate": feed_rate, "kill_rate": kill_rate}


radau_points = [0.088587959512704, 0.409466864440735, 0.787659461760847, 1.0]
time_step = 4.0
diffusion_values = [1.0, 0.5]


def collocation():
    count = len(radau_points)
    table = []
    for row in range(count):
        table.append([0.0] * count)
    for column in range(count):
        poly = [1.0]
        denom = 1.0
        for other in range(count):
            if other != column:
                longer = [0.0] * (len(poly) + 1)
                for place in range(len(poly)):
                    longer[place + 1] = longer[place + 1] + poly[place]
                    longer[place] = longer[place] - radau_points[other] * poly[place]
                poly = longer
                denom = denom * (radau_points[column] - radau_points[other])
        for row in range(count):
            point = radau_points[row]
            total = 0.0
            for place in range(len(poly)):
                total = total + poly[place] * point ** (place + 1) / (place + 1)
            table[row][column] = total / denom
    return table


def neighbours(field):
    total = jnp.roll(field, 1, 2) + jnp.roll(field, -1, 2)
    total = total + jnp.roll(field, 1, 3) + jnp.roll(field, -1, 3)
    return total + jnp.roll(field, 1, 4) + jnp.roll(field, -1, 4)


def reaction(field, feed_rate, kill_rate):
    upart = field[:, 0]
    vpart = field[:, 1]
    uvv = upart * vpart * vpart
    first = -uvv + feed_rate[None] * (1.0 - upart)
    second = uvv - (feed_rate[None] + kill_rate[None]) * vpart
    return jnp.stack([first, second], 1)


def reference(previous, feed_rate, kill_rate):
    qmatrix = jnp.asarray(collocation(), jnp.float32)
    points = jnp.asarray(radau_points, jnp.float32)[:, None, None, None, None]
    diffusion = jnp.asarray(diffusion_values, jnp.float32)[None, :, None, None, None]
    coef = time_step * points * diffusion
    start_value = previous[-1]
    iterate = previous
    for sweep in range(SWEEPS):
        laplace = neighbours(iterate) - 6.0 * iterate
        diff = diffusion * laplace
        force = diff + reaction(iterate, feed_rate, kill_rate)
        summed = jnp.einsum("mj,jsxyz->msxyz", qmatrix, force, precision=lax.Precision.HIGHEST)
        right_side = start_value[None] + time_step * (summed - points * diff)

        def jacobi(turn, current):
            return (right_side + coef * neighbours(current)) / (1.0 + 6.0 * coef)

        iterate = lax.fori_loop(0, JACOBI, jacobi, iterate)
    return iterate
```

```python
import jax
import jax.numpy as jnp
from jax import lax
from jax.experimental import pallas as pl
from jax.experimental.pallas import tpu as pltpu
from jax.sharding import PartitionSpec as P

SWEEPS = 2
JACOBI = 12


radau_points = [0.088587959512704, 0.409466864440735, 0.787659461760847, 1.0]
time_step = 4.0
diffusion_values = [1.0, 0.5]

XB, YB, ZB = 16, 32, 256
HALF = XB // 2
LANES = 128
PLANES = XB + 2 * (JACOBI + 1)
FIRST = JACOBI + 1
ROW0 = 24
ROWS = YB + 2 * ROW0
NEAR = (FIRST - 11, FIRST + XB + 11)
FAR = (FIRST - 3, FIRST + XB + 3)
NNEAR = NEAR[1] - NEAR[0]
NFAR = FAR[1] - FAR[0]
STRIP = NNEAR + NFAR


def collocation():
    count = len(radau_points)
    table = []
    for row in range(count):
        table.append([0.0] * count)
    for column in range(count):
        poly = [1.0]
        denom = 1.0
        for other in range(count):
            if other != column:
                longer = [0.0] * (len(poly) + 1)
                for place in range(len(poly)):
                    longer[place + 1] = longer[place + 1] + poly[place]
                    longer[place] = longer[place] - radau_points[other] * poly[place]
                poly = longer
                denom = denom * (radau_points[column] - radau_points[other])
        for row in range(count):
            point = radau_points[row]
            total = 0.0
            for place in range(len(poly)):
                total = total + poly[place] * point ** (place + 1) / (place + 1)
            table[row][column] = total / denom
    return table


def node_table():
    q = collocation()
    rows = []
    for n in range(4):
        a, b = n ^ 1, 3 - n
        row = [
            time_step * q[n][n], time_step * q[n][a], time_step * q[n][b],
            time_step * q[b][n], time_step * q[b][a],
            time_step * q[a][n], time_step * q[a][b],
            0.0,
        ]
        for d in diffusion_values:
            c = time_step * radau_points[n] * d
            row += [-c, c / (1.0 + 6.0 * c), 1.0 / (1.0 + 6.0 * c), d]
        rows.append(row)
    return rows


def ring(count, step):
    return [(i, (i + step) % count) for i in range(count)]


def shifted(array, axis, step):
    return lax.ppermute(array, axis, ring(lax.axis_size(axis), step))


def z_sum(c0, c1, lane):
    first, last = lane == 0, lane == LANES - 1
    up0, up1 = pltpu.roll(c0, 1, 1), pltpu.roll(c1, 1, 1)
    dn0, dn1 = pltpu.roll(c0, LANES - 1, 1), pltpu.roll(c1, LANES - 1, 1)
    low = jnp.where(first, up1, up0) + jnp.where(last, dn1, dn0)
    high = jnp.where(first, up0, up1) + jnp.where(last, dn0, dn1)
    return low, high


def force_kernel(sc, x, xlo, xhi, ylo, yhi, feed, kill,
                 fua, fub, fva, fvb, du, dv, work):
    def fill(p, carry):
        for s in range(2):
            for h in range(2):
                lanes = slice(h * LANES, (h + 1) * LANES)
                work[s, p + 1, h, 8:8 + YB, :] = x[s, p, :, lanes]
        return carry

    lax.fori_loop(0, XB, fill, 0)
    for s in range(2):
        for h in range(2):
            lanes = slice(h * LANES, (h + 1) * LANES)
            work[s, 0, h, 8:8 + YB, :] = xlo[s, 0, :, lanes]
            work[s, XB + 1, h, 8:8 + YB, :] = xhi[s, 0, :, lanes]
            for p in range(XB):
                work[s, p + 1, h, 7:8, :] = ylo[s, p:p + 1, lanes]
                work[s, p + 1, h, 8 + YB:9 + YB, :] = yhi[s, p:p + 1, lanes]
    lane = lax.broadcasted_iota(jnp.int32, (8, LANES), 1)

    def run(base, fu, fv):
        def plane(i, carry):
            p = base + i
            for t in range(YB // 8):
                r = 8 + 8 * t
                out = slice(8 * t, 8 * t + 8)
                field = []
                lap = []
                for s in range(2):
                    c = [work[s, p + 1, h, r:r + 8, :] for h in range(2)]
                    z = z_sum(c[0], c[1], lane)
                    terms = []
                    for h in range(2):
                        total = work[s, p, h, r:r + 8, :] + work[s, p + 2, h, r:r + 8, :]
                        total = total + work[s, p + 1, h, r - 1:r + 7, :]
                        total = total + work[s, p + 1, h, r + 1:r + 9, :]
                        terms.append(total + z[h] - 6.0 * c[h])
                    field.append(c)
                    lap.append(terms)
                for h in range(2):
                    lanes = slice(h * LANES, (h + 1) * LANES)
                    u, v = field[0][h], field[1][h]
                    fr, kr = feed[p, out, lanes], kill[p, out, lanes]
                    uvv = u * v * v
                    fu[i, out, lanes] = sc[11] * lap[0][h] + (fr * (1.0 - u) - uvv)
                    fv[i, out, lanes] = sc[15] * lap[1][h] + (uvv - (fr + kr) * v)
                    du[p, out, lanes] = sc[8] * lap[0][h]
                    dv[p, out, lanes] = sc[12] * lap[1][h]
            return carry

        lax.fori_loop(0, HALF, plane, 0)

    run(0, fua, fva)
    run(HALF, fub, fvb)


def forces(sc, x, xlo, xhi, ylo, yhi, feed, kill):
    half = jax.ShapeDtypeStruct((HALF, YB, ZB), jnp.float32)
    full = jax.ShapeDtypeStruct((XB, YB, ZB), jnp.float32)
    vmem = pl.BlockSpec(memory_space=pltpu.VMEM)
    return pl.pallas_call(
        force_kernel,
        out_shape=(half, half, half, half, full, full),
        in_specs=[pl.BlockSpec(memory_space=pltpu.SMEM)] + [vmem] * 7,
        out_specs=(vmem,) * 6,
        scratch_shapes=[pltpu.VMEM((2, XB + 2, 2, YB + 16, LANES), jnp.float32)],
        cost_estimate=pl.CostEstimate(flops=8_000_000, bytes_accessed=6_000_000, transcendentals=0),
        name="forces",
    )(sc, x, xlo, xhi, ylo, yhi, feed, kill)


def jacobi_kernel(species, sc, x, own, ra, rb, core, yhi, ylo, one, two, bs):
    spread = sc[8 + 4 * species + 1]
    scale = sc[8 + 4 * species + 2]
    zero = jnp.zeros((ROWS, LANES), jnp.float32)

    def clear(p, carry):
        for h in range(2):
            one[p, h] = zero
            two[p, h] = zero
        return carry

    lax.fori_loop(0, PLANES, clear, 0)

    def fill(half, recv):
        def plane(i, carry):
            p = half * HALF + i
            for h in range(2):
                lanes = slice(h * LANES, (h + 1) * LANES)
                one[FIRST + p, h, ROW0:ROW0 + YB, :] = x[0, p, :, lanes]
                bs[p, h] = scale * (own[p, :, lanes] + recv[i, :, lanes])
            return carry

        lax.fori_loop(0, HALF, plane, 0)

    fill(0, ra)
    fill(1, rb)
    lane = lax.broadcasted_iota(jnp.int32, (8, LANES), 1)

    def plane_of(src, dst, p, tiles, inside):
        for t in range(-tiles, YB // 8 + tiles):
            r = ROW0 + 8 * t
            c = [src[p, h, r:r + 8, :] for h in range(2)]
            z = z_sum(c[0], c[1], lane)
            for h in range(2):
                total = src[p - 1, h, r:r + 8, :] + src[p + 1, h, r:r + 8, :]
                total = total + (src[p, h, r - 1:r + 7, :] + src[p, h, r + 1:r + 9, :])
                new = spread * (total + z[h])
                if inside and 0 <= t < YB // 8:
                    new = new + bs[p - FIRST, h, 8 * t:8 * t + 8, :]
                dst[p, h, r:r + 8, :] = new

    def turn(src, dst, k, tiles):
        def outside(i, carry):
            plane_of(src, dst, FIRST - 1 - i, tiles, False)
            plane_of(src, dst, FIRST + XB + i, tiles, False)
            return carry

        def inside(i, carry):
            plane_of(src, dst, FIRST + i, tiles, True)
            return carry

        lax.fori_loop(0, k, outside, 0)
        lax.fori_loop(0, XB, inside, 0)

    def pair(tiles):
        def run(i, carry):
            turn(one, two, 2 * i + 1, tiles)
            turn(two, one, 2 * i + 2, tiles)
            return carry

        return run

    lax.fori_loop(0, 4, pair(1), 0)
    lax.fori_loop(4, JACOBI // 2, pair(2), 0)

    def give(p, carry):
        for h in range(2):
            lanes = slice(h * LANES, (h + 1) * LANES)
            core[p, :, lanes] = one[p + 1, h, ROW0:ROW0 + YB, :]
        return carry

    lax.fori_loop(0, XB + 2 * JACOBI, give, 0)

    def near(i, carry):
        for h in range(2):
            lanes = slice(h * LANES, (h + 1) * LANES)
            yhi[i, :, lanes] = one[NEAR[0] + i, h, ROW0 + YB:ROW0 + YB + 8, :]
            ylo[i, :, lanes] = one[NEAR[0] + i, h, ROW0 - 8:ROW0, :]
        return carry

    def far(i, carry):
        for h in range(2):
            lanes = slice(h * LANES, (h + 1) * LANES)
            yhi[NNEAR + i, :, lanes] = one[FAR[0] + i, h, ROW0 + YB + 8:ROW0 + YB + 16, :]
            ylo[NNEAR + i, :, lanes] = one[FAR[0] + i, h, ROW0 - 16:ROW0 - 8, :]
        return carry

    lax.fori_loop(0, NNEAR, near, 0)
    lax.fori_loop(0, NFAR, far, 0)


def jacobi(species, sc, x, own, ra, rb):
    vmem = pl.BlockSpec(memory_space=pltpu.VMEM)
    strip = jax.ShapeDtypeStruct((STRIP, 8, ZB), jnp.float32)
    return pl.pallas_call(
        lambda *refs: jacobi_kernel(species, *refs),
        grid=(1,),
        out_shape=(jax.ShapeDtypeStruct((XB + 2 * JACOBI, YB, ZB), jnp.float32), strip, strip),
        in_specs=[
            pl.BlockSpec(memory_space=pltpu.SMEM),
            pl.BlockSpec((1, XB, YB, ZB), lambda i: (species, 0, 0, 0)),
            vmem, vmem, vmem,
        ],
        out_specs=(vmem,) * 3,
        scratch_shapes=[
            pltpu.VMEM((PLANES, 2, ROWS, LANES), jnp.float32),
            pltpu.VMEM((PLANES, 2, ROWS, LANES), jnp.float32),
            pltpu.VMEM((XB, 2, YB, LANES), jnp.float32),
        ],
        cost_estimate=pl.CostEstimate(flops=60_000_000, bytes_accessed=5_000_000, transcendentals=0),
        name="jacobi",
    )(sc, x, own, ra, rb)


def gather_kernel(core, low, high, xlo, xhi, center):
    wide = XB + 2 * JACOBI
    for p in range(wide):
        if p < JACOBI:
            dst, q = xlo, p
        elif p < JACOBI + XB:
            dst, q = center, p - JACOBI
        else:
            dst, q = xhi, p - JACOBI - XB
        near = p + 1 - NEAR[0]
        far = p + 1 - FAR[0]
        has_near = 0 <= near < NNEAR
        has_far = 0 <= far < NFAR
        parts = [core[p, 8 * t:8 * t + 8, :] for t in range(4)]
        if has_near:
            parts[0] = parts[0] + low[near]
            parts[3] = parts[3] + high[near]
        if has_far:
            parts[1] = parts[1] + low[NNEAR + far]
            parts[2] = parts[2] + high[NNEAR + far]
        for t in range(4):
            dst[q, 8 * t:8 * t + 8, :] = parts[t]


def gathered(core, low, high):
    vmem = pl.BlockSpec(memory_space=pltpu.VMEM)
    side = jax.ShapeDtypeStruct((JACOBI, YB, ZB), jnp.float32)
    return pl.pallas_call(
        gather_kernel,
        out_shape=(side, side, jax.ShapeDtypeStruct((XB, YB, ZB), jnp.float32)),
        in_specs=[vmem] * 3,
        out_specs=(vmem,) * 3,
        cost_estimate=pl.CostEstimate(flops=1_000_000, bytes_accessed=4_000_000, transcendentals=0),
        name="gathered",
    )(core, low, high)


def final_kernel(cu, lu, hu, cv, lv, hv, out, *edges):
    gap = XB - JACOBI
    for s, (c, low, high) in enumerate(((cu, lu, hu), (cv, lv, hv))):
        for p in range(XB):
            value = c[p]
            if p < JACOBI:
                value = value + low[p]
            if p >= gap:
                value = value + high[p - gap]
            out[s, p] = value
            if edges:
                xfirst, xlast, yfirst, ylast = edges
                if p == 0:
                    xfirst[s, 0] = value
                if p == XB - 1:
                    xlast[s, 0] = value
                yfirst[s, p:p + 1, :] = value[0:1, :]
                ylast[s, p:p + 1, :] = value[YB - 1:YB, :]


def final(cu, lu, hu, cv, lv, hv, edges):
    vmem = pl.BlockSpec(memory_space=pltpu.VMEM)
    shapes = [jax.ShapeDtypeStruct((2, XB, YB, ZB), jnp.float32)]
    if edges:
        shapes += [jax.ShapeDtypeStruct((2, 1, YB, ZB), jnp.float32)] * 2
        shapes += [jax.ShapeDtypeStruct((2, XB, ZB), jnp.float32)] * 2
    return pl.pallas_call(
        final_kernel,
        out_shape=tuple(shapes),
        in_specs=[vmem] * 6,
        out_specs=(vmem,) * len(shapes),
        cost_estimate=pl.CostEstimate(flops=1_000_000, bytes_accessed=4_000_000, transcendentals=0),
        name="final",
    )(cu, lu, hu, cv, lv, hv)


PAIR_A = [(0, 1), (1, 0), (2, 3), (3, 2)]
PAIR_B = [(0, 3), (3, 0), (1, 2), (2, 1)]


def body(previous, feed_rate, kill_rate):
    node = lax.axis_index("node")
    sc = jnp.asarray(node_table(), jnp.float32)[node]
    x = previous[0]
    sent_a = lax.ppermute(x[:, :HALF], "node", [(3, 2)])
    sent_b = lax.ppermute(x[:, HALF:], "node", [(3, 0)])
    last = node == 3
    edges = (x[:, :1], x[:, XB - 1:], x[:, :, 0], x[:, :, YB - 1])
    for sweep in range(SWEEPS):
        xfirst, xlast, yfirst, ylast = edges
        xlo = shifted(xlast, "sx", 1)
        xhi = shifted(xfirst, "sx", -1)
        ylo = shifted(ylast, "sy", 1)
        yhi = shifted(yfirst, "sy", -1)
        if sweep == 0:
            start_a = jnp.where(last, x[:, :HALF], sent_a)
            start_b = jnp.where(last, x[:, HALF:], sent_b)
        fua, fub, fva, fvb, du, dv = forces(sc, x, xlo, xhi, ylo, yhi, feed_rate, kill_rate)
        cores = []
        for s, (fa, fb, d) in enumerate(((fua, fub, du), (fva, fvb, dv))):
            ga = lax.ppermute(fa, "node", PAIR_A)
            gb = lax.ppermute(fb, "node", PAIR_B)
            ra = lax.ppermute(sc[3] * fa + sc[4] * ga + start_a[s], "node", PAIR_B)
            rb = lax.ppermute(sc[5] * fb + sc[6] * gb + start_b[s], "node", PAIR_A)
            own = jnp.concatenate(
                [
                    sc[0] * fa + sc[1] * ga + start_a[s] + d[:HALF],
                    sc[0] * fb + sc[2] * gb + start_b[s] + d[HALF:],
                ],
                0,
            )
            core, up, down = jacobi(s, sc, x, own, ra, rb)
            low = shifted(up, "sy", 1)
            high = shifted(down, "sy", -1)
            left, right, center = gathered(core, low, high)
            cores += [center, shifted(right, "sx", 1), shifted(left, "sx", -1)]
        x, *edges = final(*cores, sweep + 1 < SWEEPS)
    return x[None]


def solution(mesh):
    return jax.shard_map(
        body,
        mesh=mesh,
        in_specs=(P("node", None, "sx", "sy", None), P("sx", "sy", None), P("sx", "sy", None)),
        out_specs=P("node", None, "sx", "sy", None),
        check_vma=False,
    )
```

```python
import jax
import jax.numpy as jnp
import numpy as np
from jax import lax
from jax.experimental import pallas as pl
from jax.experimental.pallas import tpu as pltpu
from jax.sharding import PartitionSpec as P

SWEEPS = 2
JACOBI = 12


radau_points = [0.088587959512704, 0.409466864440735, 0.787659461760847, 1.0]
time_step = 4.0
diffusion_values = [1.0, 0.5]

XB, YB, ZB = 16, 32, 256
HALF = XB // 2
LANES = 128
PLANES = XB + 2 * (JACOBI + 1)
FIRST = JACOBI + 1
ROW0 = 24
ROWS = YB + 2 * ROW0
NEAR = (FIRST - 11, FIRST + XB + 11)
FAR = (FIRST - 3, FIRST + XB + 3)
NNEAR = NEAR[1] - NEAR[0]
NFAR = FAR[1] - FAR[0]
STRIP = NNEAR + NFAR


def collocation():
    count = len(radau_points)
    table = []
    for row in range(count):
        table.append([0.0] * count)
    for column in range(count):
        poly = [1.0]
        denom = 1.0
        for other in range(count):
            if other != column:
                longer = [0.0] * (len(poly) + 1)
                for place in range(len(poly)):
                    longer[place + 1] = longer[place + 1] + poly[place]
                    longer[place] = longer[place] - radau_points[other] * poly[place]
                poly = longer
                denom = denom * (radau_points[column] - radau_points[other])
        for row in range(count):
            point = radau_points[row]
            total = 0.0
            for place in range(len(poly)):
                total = total + poly[place] * point ** (place + 1) / (place + 1)
            table[row][column] = total / denom
    return table


def node_table():
    q = collocation()
    rows = []
    for n in range(4):
        a, b = n ^ 1, 3 - n
        row = [
            time_step * q[n][n], time_step * q[n][a], time_step * q[n][b],
            time_step * q[b][n], time_step * q[b][a],
            time_step * q[a][n], time_step * q[a][b],
            0.0,
        ]
        for d in diffusion_values:
            c = time_step * radau_points[n] * d
            row += [-c, c / (1.0 + 6.0 * c), 1.0 / (1.0 + 6.0 * c), d]
        rows.append(row)
    return rows


def fourier():
    place = np.arange(ZB)[:, None]
    wave = np.arange(ZB)
    sine = wave > ZB // 2
    wave = np.where(sine, wave - ZB // 2, wave)
    angle = 2.0 * np.pi * ((place * wave) % ZB) / ZB
    basis = np.where(sine, np.sin(angle), np.cos(angle)) * np.sqrt(2.0 / ZB)
    basis[:, 0] = np.sqrt(1.0 / ZB)
    basis[:, ZB // 2] = np.cos(angle[:, ZB // 2]) * np.sqrt(1.0 / ZB)
    sums = np.broadcast_to(2.0 * np.cos(2.0 * np.pi * wave / ZB), (8, ZB))
    return basis.astype(np.float32), sums.astype(np.float32)


def ring(count, step):
    return [(i, (i + step) % count) for i in range(count)]


def shifted(array, axis, step):
    return lax.ppermute(array, axis, ring(lax.axis_size(axis), step))


def z_sum(c0, c1, lane):
    first, last = lane == 0, lane == LANES - 1
    up0, up1 = pltpu.roll(c0, 1, 1), pltpu.roll(c1, 1, 1)
    dn0, dn1 = pltpu.roll(c0, LANES - 1, 1), pltpu.roll(c1, LANES - 1, 1)
    low = jnp.where(first, up1, up0) + jnp.where(last, dn1, dn0)
    high = jnp.where(first, up0, up1) + jnp.where(last, dn0, dn1)
    return low, high


def force_kernel(sc, x, xlo, xhi, ylo, yhi, feed, kill,
                 fua, fub, fva, fvb, du, dv, work):
    def fill(p, carry):
        for s in range(2):
            for h in range(2):
                lanes = slice(h * LANES, (h + 1) * LANES)
                work[s, p + 1, h, 8:8 + YB, :] = x[s, p, :, lanes]
        return carry

    lax.fori_loop(0, XB, fill, 0)
    for s in range(2):
        for h in range(2):
            lanes = slice(h * LANES, (h + 1) * LANES)
            work[s, 0, h, 8:8 + YB, :] = xlo[s, 0, :, lanes]
            work[s, XB + 1, h, 8:8 + YB, :] = xhi[s, 0, :, lanes]
            for p in range(XB):
                work[s, p + 1, h, 7:8, :] = ylo[s, p:p + 1, lanes]
                work[s, p + 1, h, 8 + YB:9 + YB, :] = yhi[s, p:p + 1, lanes]
    lane = lax.broadcasted_iota(jnp.int32, (8, LANES), 1)

    def run(base, fu, fv):
        def plane(i, carry):
            p = base + i
            for t in range(YB // 8):
                r = 8 + 8 * t
                out = slice(8 * t, 8 * t + 8)
                field = []
                lap = []
                for s in range(2):
                    c = [work[s, p + 1, h, r:r + 8, :] for h in range(2)]
                    z = z_sum(c[0], c[1], lane)
                    terms = []
                    for h in range(2):
                        total = work[s, p, h, r:r + 8, :] + work[s, p + 2, h, r:r + 8, :]
                        total = total + work[s, p + 1, h, r - 1:r + 7, :]
                        total = total + work[s, p + 1, h, r + 1:r + 9, :]
                        terms.append(total + z[h] - 6.0 * c[h])
                    field.append(c)
                    lap.append(terms)
                for h in range(2):
                    lanes = slice(h * LANES, (h + 1) * LANES)
                    u, v = field[0][h], field[1][h]
                    fr, kr = feed[p, out, lanes], kill[p, out, lanes]
                    uvv = u * v * v
                    fu[i, out, lanes] = sc[11] * lap[0][h] + (fr * (1.0 - u) - uvv)
                    fv[i, out, lanes] = sc[15] * lap[1][h] + (uvv - (fr + kr) * v)
                    du[p, out, lanes] = sc[8] * lap[0][h]
                    dv[p, out, lanes] = sc[12] * lap[1][h]
            return carry

        lax.fori_loop(0, HALF, plane, 0)

    run(0, fua, fva)
    run(HALF, fub, fvb)


def forces(sc, x, xlo, xhi, ylo, yhi, feed, kill):
    half = jax.ShapeDtypeStruct((HALF, YB, ZB), jnp.float32)
    full = jax.ShapeDtypeStruct((XB, YB, ZB), jnp.float32)
    vmem = pl.BlockSpec(memory_space=pltpu.VMEM)
    return pl.pallas_call(
        force_kernel,
        out_shape=(half, half, half, half, full, full),
        in_specs=[pl.BlockSpec(memory_space=pltpu.SMEM)] + [vmem] * 7,
        out_specs=(vmem,) * 6,
        scratch_shapes=[pltpu.VMEM((2, XB + 2, 2, YB + 16, LANES), jnp.float32)],
        cost_estimate=pl.CostEstimate(flops=8_000_000, bytes_accessed=6_000_000, transcendentals=0),
        name="forces",
    )(sc, x, xlo, xhi, ylo, yhi, feed, kill)


def jacobi_kernel(species, sc, basis, sums, x, own, ra, rb, core, yhi, ylo, one, two, bs):
    spread = sc[8 + 4 * species + 1]
    scale = sc[8 + 4 * species + 2]
    zero = jnp.zeros((ROWS, LANES), jnp.float32)

    def clear(p, carry):
        for h in range(2):
            one[p, h] = zero
            two[p, h] = zero
            bs[p, h] = zero[:YB]
        return carry

    lax.fori_loop(0, PLANES, clear, 0)

    def modes(values):
        flat = values.reshape(-1, ZB)
        done = jnp.dot(flat, basis[...], precision=lax.Precision.HIGHEST,
                       preferred_element_type=jnp.float32)
        return done.reshape(values.shape)

    def fill(half, recv):
        def planes(i, carry):
            p = half * HALF + i * 4
            xh = modes(x[0, pl.ds(p, 4)])
            bh = modes(own[pl.ds(p, 4)] + recv[pl.ds(i * 4, 4)])
            for h in range(2):
                lanes = slice(h * LANES, (h + 1) * LANES)
                for j in range(4):
                    one[FIRST + p + j, h, ROW0:ROW0 + YB, :] = xh[j, :, lanes]
                    bs[FIRST + p + j, h] = scale * bh[j, :, lanes]
            return carry

        lax.fori_loop(0, HALF // 4, planes, 0)

    fill(0, ra)
    fill(1, rb)
    turned = [spread * sums[:, h * LANES:(h + 1) * LANES] for h in range(2)]

    def one_plane(src, dst, p, group, carry):
        count = 2 * len(group)
        before, here = carry[:count], carry[count:]
        after = []
        for t in group:
            r = ROW0 + 8 * t
            after += [src[p + 1, h, r:r + 8, :] for h in range(2)]
        for j, t in enumerate(group):
            r = ROW0 + 8 * t
            for h in range(2):
                i = 2 * j + h
                total = before[i] + after[i]
                total = total + (src[p, h, r - 1:r + 7, :] + src[p, h, r + 1:r + 9, :])
                new = spread * total + turned[h] * here[i]
                if 0 <= t < YB // 8:
                    new = new + bs[p, h, 8 * t:8 * t + 8, :]
                dst[p, h, r:r + 8, :] = new
        return (*here, *after)

    def turn(src, dst, k, tiles):
        wide = (k + 1) // 2
        first = FIRST - 2 * wide
        span = list(range(-tiles, YB // 8 + tiles))
        for group in (span[:len(span) // 2], span[len(span) // 2:]):

            def step(i, carry, group=group):
                for j in range(4):
                    carry = one_plane(src, dst, first + 4 * i + j, group, carry)
                return carry

            carry = (jnp.zeros((8, LANES), jnp.float32),) * (4 * len(group))
            lax.fori_loop(0, XB // 4 + wide, step, carry)

    def pair(tiles):
        def run(i, carry):
            turn(one, two, 2 * i + 1, tiles)
            turn(two, one, 2 * i + 2, tiles)
            return carry

        return run

    lax.fori_loop(0, 4, pair(1), 0)
    lax.fori_loop(4, JACOBI // 2, pair(2), 0)

    def give(p, carry):
        for h in range(2):
            lanes = slice(h * LANES, (h + 1) * LANES)
            core[p, :, lanes] = one[p + 1, h, ROW0:ROW0 + YB, :]
        return carry

    lax.fori_loop(0, XB + 2 * JACOBI, give, 0)

    def near(i, carry):
        for h in range(2):
            lanes = slice(h * LANES, (h + 1) * LANES)
            yhi[i, :, lanes] = one[NEAR[0] + i, h, ROW0 + YB:ROW0 + YB + 8, :]
            ylo[i, :, lanes] = one[NEAR[0] + i, h, ROW0 - 8:ROW0, :]
        return carry

    def far(i, carry):
        for h in range(2):
            lanes = slice(h * LANES, (h + 1) * LANES)
            yhi[NNEAR + i, :, lanes] = one[FAR[0] + i, h, ROW0 + YB + 8:ROW0 + YB + 16, :]
            ylo[NNEAR + i, :, lanes] = one[FAR[0] + i, h, ROW0 - 16:ROW0 - 8, :]
        return carry

    lax.fori_loop(0, NNEAR, near, 0)
    lax.fori_loop(0, NFAR, far, 0)


def jacobi(species, sc, basis, sums, x, own, ra, rb):
    vmem = pl.BlockSpec(memory_space=pltpu.VMEM)
    strip = jax.ShapeDtypeStruct((STRIP, 8, ZB), jnp.float32)
    return pl.pallas_call(
        lambda *refs: jacobi_kernel(species, *refs),
        grid=(1,),
        out_shape=(jax.ShapeDtypeStruct((XB + 2 * JACOBI, YB, ZB), jnp.float32), strip, strip),
        in_specs=[
            pl.BlockSpec(memory_space=pltpu.SMEM),
            vmem, vmem,
            pl.BlockSpec((1, XB, YB, ZB), lambda i: (species, 0, 0, 0)),
            vmem, vmem, vmem,
        ],
        out_specs=(vmem,) * 3,
        scratch_shapes=[
            pltpu.VMEM((PLANES, 2, ROWS, LANES), jnp.float32),
            pltpu.VMEM((PLANES, 2, ROWS, LANES), jnp.float32),
            pltpu.VMEM((PLANES, 2, YB, LANES), jnp.float32),
        ],
        cost_estimate=pl.CostEstimate(flops=60_000_000, bytes_accessed=5_000_000, transcendentals=0),
        name="jacobi",
    )(sc, basis, sums, x, own, ra, rb)


def gather_kernel(core, low, high, xlo, xhi, center):
    wide = XB + 2 * JACOBI
    for p in range(wide):
        if p < JACOBI:
            dst, q = xlo, p
        elif p < JACOBI + XB:
            dst, q = center, p - JACOBI
        else:
            dst, q = xhi, p - JACOBI - XB
        near = p + 1 - NEAR[0]
        far = p + 1 - FAR[0]
        has_near = 0 <= near < NNEAR
        has_far = 0 <= far < NFAR
        parts = [core[p, 8 * t:8 * t + 8, :] for t in range(4)]
        if has_near:
            parts[0] = parts[0] + low[near]
            parts[3] = parts[3] + high[near]
        if has_far:
            parts[1] = parts[1] + low[NNEAR + far]
            parts[2] = parts[2] + high[NNEAR + far]
        for t in range(4):
            dst[q, 8 * t:8 * t + 8, :] = parts[t]


def gathered(core, low, high):
    vmem = pl.BlockSpec(memory_space=pltpu.VMEM)
    side = jax.ShapeDtypeStruct((JACOBI, YB, ZB), jnp.float32)
    return pl.pallas_call(
        gather_kernel,
        out_shape=(side, side, jax.ShapeDtypeStruct((XB, YB, ZB), jnp.float32)),
        in_specs=[vmem] * 3,
        out_specs=(vmem,) * 3,
        cost_estimate=pl.CostEstimate(flops=1_000_000, bytes_accessed=4_000_000, transcendentals=0),
        name="gathered",
    )(core, low, high)


def final_kernel(basis, cu, lu, hu, cv, lv, hv, out, *edges):
    gap = XB - JACOBI
    for s, (c, low, high) in enumerate(((cu, lu, hu), (cv, lv, hv))):
        for q in range(0, XB, 4):
            parts = []
            for p in range(q, q + 4):
                value = c[p]
                if p < JACOBI:
                    value = value + low[p]
                if p >= gap:
                    value = value + high[p - gap]
                parts.append(value)
            flat = jnp.concatenate(parts, 0)
            done = lax.dot_general(flat, basis[...], (((1,), (1,)), ((), ())),
                                   precision=lax.Precision.HIGHEST,
                                   preferred_element_type=jnp.float32)
            for p in range(q, q + 4):
                value = done[(p - q) * YB:(p - q + 1) * YB]
                out[s, p] = value
                if edges:
                    xfirst, xlast, yfirst, ylast = edges
                    if p == 0:
                        xfirst[s, 0] = value
                    if p == XB - 1:
                        xlast[s, 0] = value
                    yfirst[s, p:p + 1, :] = value[0:1, :]
                    ylast[s, p:p + 1, :] = value[YB - 1:YB, :]


def final(basis, cu, lu, hu, cv, lv, hv, edges):
    vmem = pl.BlockSpec(memory_space=pltpu.VMEM)
    shapes = [jax.ShapeDtypeStruct((2, XB, YB, ZB), jnp.float32)]
    if edges:
        shapes += [jax.ShapeDtypeStruct((2, 1, YB, ZB), jnp.float32)] * 2
        shapes += [jax.ShapeDtypeStruct((2, XB, ZB), jnp.float32)] * 2
    return pl.pallas_call(
        final_kernel,
        out_shape=tuple(shapes),
        in_specs=[vmem] * 7,
        out_specs=(vmem,) * len(shapes),
        cost_estimate=pl.CostEstimate(flops=1_000_000, bytes_accessed=4_000_000, transcendentals=0),
        name="final",
    )(basis, cu, lu, hu, cv, lv, hv)


PAIR_A = [(0, 1), (1, 0), (2, 3), (3, 2)]
PAIR_B = [(0, 3), (3, 0), (1, 2), (2, 1)]


def body(previous, feed_rate, kill_rate):
    node = lax.axis_index("node")
    sc = jnp.asarray(node_table(), jnp.float32)[node]
    basis, sums = map(jnp.asarray, fourier())
    x = previous[0]
    sent_a = lax.ppermute(x[:, :HALF], "node", [(3, 2)])
    sent_b = lax.ppermute(x[:, HALF:], "node", [(3, 0)])
    last = node == 3
    edges = (x[:, :1], x[:, XB - 1:], x[:, :, 0], x[:, :, YB - 1])
    for sweep in range(SWEEPS):
        xfirst, xlast, yfirst, ylast = edges
        xlo = shifted(xlast, "sx", 1)
        xhi = shifted(xfirst, "sx", -1)
        ylo = shifted(ylast, "sy", 1)
        yhi = shifted(yfirst, "sy", -1)
        if sweep == 0:
            start_a = jnp.where(last, x[:, :HALF], sent_a)
            start_b = jnp.where(last, x[:, HALF:], sent_b)
        fua, fub, fva, fvb, du, dv = forces(sc, x, xlo, xhi, ylo, yhi, feed_rate, kill_rate)
        cores = []
        for s, (fa, fb, d) in enumerate(((fua, fub, du), (fva, fvb, dv))):
            ga = lax.ppermute(fa, "node", PAIR_A)
            gb = lax.ppermute(fb, "node", PAIR_B)
            ra = lax.ppermute(sc[3] * fa + sc[4] * ga + start_a[s], "node", PAIR_B)
            rb = lax.ppermute(sc[5] * fb + sc[6] * gb + start_b[s], "node", PAIR_A)
            own = jnp.concatenate(
                [
                    sc[0] * fa + sc[1] * ga + start_a[s] + d[:HALF],
                    sc[0] * fb + sc[2] * gb + start_b[s] + d[HALF:],
                ],
                0,
            )
            core, up, down = jacobi(s, sc, basis, sums, x, own, ra, rb)
            low = shifted(up, "sy", 1)
            high = shifted(down, "sy", -1)
            left, right, center = gathered(core, low, high)
            cores += [center, shifted(right, "sx", 1), shifted(left, "sx", -1)]
        x, *edges = final(basis, *cores, sweep + 1 < SWEEPS)
    return x[None]


def solution(mesh):
    return jax.shard_map(
        body,
        mesh=mesh,
        in_specs=(P("node", None, "sx", "sy", None), P("sx", "sy", None), P("sx", "sy", None)),
        out_specs=P("node", None, "sx", "sy", None),
        check_vma=False,
    )
```

```python
import jax
import jax.numpy as jnp
import numpy as np
from jax import lax
from jax.experimental import pallas as pl
from jax.experimental.pallas import tpu as pltpu
from jax.sharding import PartitionSpec as P

SWEEPS = 2
JACOBI = 12


radau_points = [0.088587959512704, 0.409466864440735, 0.787659461760847, 1.0]
time_step = 4.0
diffusion_values = [1.0, 0.5]

XB, YB, ZB = 16, 32, 256
HALF = XB // 2
LANES = 128
PLANES = XB + 2 * (JACOBI + 1)
FIRST = JACOBI + 1
ROW0 = 24
ROWS = YB + 2 * ROW0
NEAR = (FIRST - 11, FIRST + XB + 11)
FAR = (FIRST - 3, FIRST + XB + 3)
NNEAR = NEAR[1] - NEAR[0]
NFAR = FAR[1] - FAR[0]
STRIP = NNEAR + NFAR


def collocation():
    count = len(radau_points)
    table = []
    for row in range(count):
        table.append([0.0] * count)
    for column in range(count):
        poly = [1.0]
        denom = 1.0
        for other in range(count):
            if other != column:
                longer = [0.0] * (len(poly) + 1)
                for place in range(len(poly)):
                    longer[place + 1] = longer[place + 1] + poly[place]
                    longer[place] = longer[place] - radau_points[other] * poly[place]
                poly = longer
                denom = denom * (radau_points[column] - radau_points[other])
        for row in range(count):
            point = radau_points[row]
            total = 0.0
            for place in range(len(poly)):
                total = total + poly[place] * point ** (place + 1) / (place + 1)
            table[row][column] = total / denom
    return table


def node_table():
    q = collocation()
    rows = []
    for n in range(4):
        a, b = n ^ 1, 3 - n
        row = [
            time_step * q[n][n], time_step * q[n][a], time_step * q[n][b],
            time_step * q[b][n], time_step * q[b][a],
            time_step * q[a][n], time_step * q[a][b],
            1.0 if n == 3 else 0.0,
        ]
        for d in diffusion_values:
            c = time_step * radau_points[n] * d
            row += [-c, c / (1.0 + 6.0 * c), 1.0 / (1.0 + 6.0 * c), d]
        rows.append(row)
    return rows


def fourier():
    place = np.arange(ZB)[:, None]
    wave = np.arange(ZB)
    sine = wave > ZB // 2
    wave = np.where(sine, wave - ZB // 2, wave)
    angle = 2.0 * np.pi * ((place * wave) % ZB) / ZB
    basis = np.where(sine, np.sin(angle), np.cos(angle)) * np.sqrt(2.0 / ZB)
    basis[:, 0] = np.sqrt(1.0 / ZB)
    basis[:, ZB // 2] = np.cos(angle[:, ZB // 2]) * np.sqrt(1.0 / ZB)
    sums = np.broadcast_to(2.0 * np.cos(2.0 * np.pi * wave / ZB), (8, ZB))
    return basis.astype(np.float32), sums.astype(np.float32)


def ring(count, step):
    return [(i, (i + step) % count) for i in range(count)]


def shifted(array, axis, step):
    return lax.ppermute(array, axis, ring(lax.axis_size(axis), step))


def call(kernel, outs, args, scratch=(), flops=1_000_000, name=None):
    vmem = pl.BlockSpec(memory_space=pltpu.VMEM)
    smem = pl.BlockSpec(memory_space=pltpu.SMEM)
    return pl.pallas_call(
        kernel,
        out_shape=tuple(outs),
        in_specs=[smem] + [vmem] * (len(args) - 1),
        out_specs=(vmem,) * len(outs),
        scratch_shapes=list(scratch),
        compiler_params=pltpu.CompilerParams(vmem_limit_bytes=24 * 2**20),
        cost_estimate=pl.CostEstimate(flops=flops, bytes_accessed=1_000_000, transcendentals=0),
        name=name,
    )(args[0], *(pltpu.with_memory_space_constraint(a, pltpu.VMEM) for a in args[1:]))


def local(*shape):
    return pltpu.VMEM(shape, jnp.float32)


def z_sum(c0, c1, lane):
    first, last = lane == 0, lane == LANES - 1
    up0, up1 = pltpu.roll(c0, 1, 1), pltpu.roll(c1, 1, 1)
    dn0, dn1 = pltpu.roll(c0, LANES - 1, 1), pltpu.roll(c1, LANES - 1, 1)
    low = jnp.where(first, up1, up0) + jnp.where(last, dn1, dn0)
    high = jnp.where(first, up0, up1) + jnp.where(last, dn0, dn1)
    return low, high


def force_kernel(sc, xu, xv, xlo, xhi, ylo, yhi, feed, kill,
                 fua, fub, fva, fvb, dua, dub, dva, dvb, work):
    def fill(p, carry):
        for s, x in enumerate((xu, xv)):
            for h in range(2):
                lanes = slice(h * LANES, (h + 1) * LANES)
                work[s, p + 1, h, 8:8 + YB, :] = x[p, :, lanes]
        return carry

    lax.fori_loop(0, XB, fill, 0)
    for s in range(2):
        for h in range(2):
            lanes = slice(h * LANES, (h + 1) * LANES)
            work[s, 0, h, 8:8 + YB, :] = xlo[s, :, lanes]
            work[s, XB + 1, h, 8:8 + YB, :] = xhi[s, :, lanes]
            for p in range(XB):
                work[s, p + 1, h, 7:8, :] = ylo[s, p:p + 1, lanes]
                work[s, p + 1, h, 8 + YB:9 + YB, :] = yhi[s, p:p + 1, lanes]
    lane = lax.broadcasted_iota(jnp.int32, (8, LANES), 1)

    def run(base, fu, fv, du, dv):
        def plane(i, carry):
            p = base + i
            for t in range(YB // 8):
                r = 8 + 8 * t
                out = slice(8 * t, 8 * t + 8)
                field = []
                lap = []
                for s in range(2):
                    c = [work[s, p + 1, h, r:r + 8, :] for h in range(2)]
                    z = z_sum(c[0], c[1], lane)
                    terms = []
                    for h in range(2):
                        total = work[s, p, h, r:r + 8, :] + work[s, p + 2, h, r:r + 8, :]
                        total = total + work[s, p + 1, h, r - 1:r + 7, :]
                        total = total + work[s, p + 1, h, r + 1:r + 9, :]
                        terms.append(total + z[h] - 6.0 * c[h])
                    field.append(c)
                    lap.append(terms)
                for h in range(2):
                    lanes = slice(h * LANES, (h + 1) * LANES)
                    u, v = field[0][h], field[1][h]
                    fr, kr = feed[p, out, lanes], kill[p, out, lanes]
                    uvv = u * v * v
                    fu[i, out, lanes] = sc[11] * lap[0][h] + (fr * (1.0 - u) - uvv)
                    fv[i, out, lanes] = sc[15] * lap[1][h] + (uvv - (fr + kr) * v)
                    du[i, out, lanes] = sc[8] * lap[0][h]
                    dv[i, out, lanes] = sc[12] * lap[1][h]
            return carry

        lax.fori_loop(0, HALF, plane, 0)

    run(0, fua, fva, dua, dva)
    run(HALF, fub, fvb, dub, dvb)


def forces(*args):
    return call(
        force_kernel,
        [local(HALF, YB, ZB)] * 8,
        args,
        [pltpu.VMEM((2, XB + 2, 2, YB + 16, LANES), jnp.float32)],
        flops=8_000_000,
        name="forces",
    )


def partial_kernel(species, sc, fa, fb, ga, gb, na, nb, x0, sa, sb):
    def plane(p, carry):
        low = na[species, p] + sc[7] * x0[p]
        high = nb[species, p] + sc[7] * x0[HALF + p]
        sa[p] = sc[3] * fa[p] + sc[4] * ga[p] + low
        sb[p] = sc[5] * fb[p] + sc[6] * gb[p] + high
        return carry

    lax.fori_loop(0, HALF, plane, 0)


def partial(species, *args):
    return call(
        lambda *refs: partial_kernel(species, *refs),
        [local(HALF, YB, ZB)] * 2,
        args,
        name="partial",
    )


def jacobi_kernel(species, sc, basis, sums, x, x0, na, nb, fa, fb, ga, gb, da, db, ra, rb,
                  core, yhi, ylo, one, two, bs):
    spread = sc[8 + 4 * species + 1]
    scale = sc[8 + 4 * species + 2]
    zero = jnp.zeros((ROWS, LANES), jnp.float32)

    def clear(p, carry):
        for h in range(2):
            one[p, h] = zero
            two[p, h] = zero
            bs[p, h] = zero[:YB]
        return carry

    lax.fori_loop(0, PLANES, clear, 0)

    def modes(values):
        flat = values.reshape(-1, ZB)
        done = jnp.dot(flat, basis[...], precision=lax.Precision.HIGHEST,
                       preferred_element_type=jnp.float32)
        return done.reshape(values.shape)

    def fill(half, f, g, d, n, recv, weight):
        def planes(i, carry):
            p = half * HALF + i * 4
            part = pl.ds(i * 4, 4)
            xh = modes(x[pl.ds(p, 4)])
            own = sc[0] * f[part] + sc[weight] * g[part] + d[part]
            own = own + (n[species, part] + sc[7] * x0[pl.ds(p, 4)])
            bh = modes(own + recv[part])
            for h in range(2):
                lanes = slice(h * LANES, (h + 1) * LANES)
                for j in range(4):
                    one[FIRST + p + j, h, ROW0:ROW0 + YB, :] = xh[j, :, lanes]
                    bs[FIRST + p + j, h] = scale * bh[j, :, lanes]
            return carry

        lax.fori_loop(0, HALF // 4, planes, 0)

    fill(0, fa, ga, da, na, ra, 1)
    fill(1, fb, gb, db, nb, rb, 2)
    turned = [spread * sums[:, h * LANES:(h + 1) * LANES] for h in range(2)]

    def one_plane(src, dst, p, group, carry):
        count = 2 * len(group)
        before, here = carry[:count], carry[count:]
        after = []
        for t in group:
            r = ROW0 + 8 * t
            after += [src[p + 1, h, r:r + 8, :] for h in range(2)]
        for j, t in enumerate(group):
            r = ROW0 + 8 * t
            for h in range(2):
                i = 2 * j + h
                total = before[i] + after[i]
                total = total + (src[p, h, r - 1:r + 7, :] + src[p, h, r + 1:r + 9, :])
                new = spread * total + turned[h] * here[i]
                if 0 <= t < YB // 8:
                    new = new + bs[p, h, 8 * t:8 * t + 8, :]
                dst[p, h, r:r + 8, :] = new
        return (*here, *after)

    def turn(src, dst, k, tiles):
        wide = (k + 1) // 2
        first = FIRST - 2 * wide
        span = list(range(-tiles, YB // 8 + tiles))
        for group in (span[:len(span) // 2], span[len(span) // 2:]):

            def step(i, carry, group=group):
                for j in range(4):
                    carry = one_plane(src, dst, first + 4 * i + j, group, carry)
                return carry

            carry = (jnp.zeros((8, LANES), jnp.float32),) * (4 * len(group))
            lax.fori_loop(0, XB // 4 + wide, step, carry)

    def pair(tiles):
        def run(i, carry):
            turn(one, two, 2 * i + 1, tiles)
            turn(two, one, 2 * i + 2, tiles)
            return carry

        return run

    lax.fori_loop(0, 4, pair(1), 0)
    lax.fori_loop(4, JACOBI // 2, pair(2), 0)

    def give(p, carry):
        for h in range(2):
            lanes = slice(h * LANES, (h + 1) * LANES)
            core[p, :, lanes] = one[p + 1, h, ROW0:ROW0 + YB, :]
        return carry

    lax.fori_loop(0, XB + 2 * JACOBI, give, 0)

    def near(i, carry):
        for h in range(2):
            lanes = slice(h * LANES, (h + 1) * LANES)
            yhi[i, :, lanes] = one[NEAR[0] + i, h, ROW0 + YB:ROW0 + YB + 8, :]
            ylo[i, :, lanes] = one[NEAR[0] + i, h, ROW0 - 8:ROW0, :]
        return carry

    def far(i, carry):
        for h in range(2):
            lanes = slice(h * LANES, (h + 1) * LANES)
            yhi[NNEAR + i, :, lanes] = one[FAR[0] + i, h, ROW0 + YB + 8:ROW0 + YB + 16, :]
            ylo[NNEAR + i, :, lanes] = one[FAR[0] + i, h, ROW0 - 16:ROW0 - 8, :]
        return carry

    lax.fori_loop(0, NNEAR, near, 0)
    lax.fori_loop(0, NFAR, far, 0)


def jacobi(species, *args):
    return call(
        lambda *refs: jacobi_kernel(species, *refs),
        [local(XB + 2 * JACOBI, YB, ZB)] + [local(STRIP, 8, ZB)] * 2,
        args,
        [
            pltpu.VMEM((PLANES, 2, ROWS, LANES), jnp.float32),
            pltpu.VMEM((PLANES, 2, ROWS, LANES), jnp.float32),
            pltpu.VMEM((PLANES, 2, YB, LANES), jnp.float32),
        ],
        flops=60_000_000,
        name="jacobi",
    )


def gather_kernel(sc, core, low, high, xlo, xhi, center):
    wide = XB + 2 * JACOBI
    for p in range(wide):
        if p < JACOBI:
            dst, q = xlo, p
        elif p < JACOBI + XB:
            dst, q = center, p - JACOBI
        else:
            dst, q = xhi, p - JACOBI - XB
        near = p + 1 - NEAR[0]
        far = p + 1 - FAR[0]
        has_near = 0 <= near < NNEAR
        has_far = 0 <= far < NFAR
        parts = [core[p, 8 * t:8 * t + 8, :] for t in range(4)]
        if has_near:
            parts[0] = parts[0] + low[near]
            parts[3] = parts[3] + high[near]
        if has_far:
            parts[1] = parts[1] + low[NNEAR + far]
            parts[2] = parts[2] + high[NNEAR + far]
        for t in range(4):
            dst[q, 8 * t:8 * t + 8, :] = parts[t]


def gathered(*args):
    return call(
        gather_kernel,
        [local(JACOBI, YB, ZB)] * 2 + [local(XB, YB, ZB)],
        args,
        name="gathered",
    )


def back(basis, c, low, high, total, give):
    gap = XB - JACOBI

    def add(p, carry):
        total[p] = c[p]
        return carry

    def add_low(p, carry):
        total[p] += low[p]
        return carry

    def add_high(p, carry):
        total[gap + p] += high[p]
        return carry

    lax.fori_loop(0, XB, add, 0)
    lax.fori_loop(0, JACOBI, add_low, 0)
    lax.fori_loop(0, JACOBI, add_high, 0)

    def turn(i, carry):
        flat = total[pl.ds(8 * i, 8)].reshape(8 * YB, ZB)
        done = lax.dot_general(flat, basis[...], (((1,), (1,)), ((), ())),
                               precision=lax.Precision.HIGHEST,
                               preferred_element_type=jnp.float32)
        give(8 * i, done.reshape(8, YB, ZB))
        return carry

    lax.fori_loop(0, XB // 8, turn, 0)


def first_kernel(sc, basis, c, low, high, out, total):
    def give(p, value):
        out[pl.ds(p, 8)] = value

    back(basis, c, low, high, total, give)


def middle_kernel(sc, basis, c, low, high, xu, out, xfirst, xlast, yfirst, ylast, total):
    def give(p, value):
        out[pl.ds(p, 8)] = value

    back(basis, c, low, high, total, give)
    for s, x in enumerate((xu, out)):
        xfirst[s] = x[0]
        xlast[s] = x[XB - 1]
        for p in range(XB):
            yfirst[s, p:p + 1, :] = x[p, 0:1, :]
            ylast[s, p:p + 1, :] = x[p, YB - 1:YB, :]


def last_kernel(sc, basis, c, low, high, xu, out, total):
    def give(p, value):
        out[1, pl.ds(p, 8)] = value

    def copy(p, carry):
        out[0, p] = xu[p]
        return carry

    lax.fori_loop(0, XB, copy, 0)
    back(basis, c, low, high, total, give)


TOTAL = [pltpu.VMEM((XB, YB, ZB), jnp.float32)]


def first(*args):
    return call(first_kernel, [local(XB, YB, ZB)], args, TOTAL, name="first")[0]


def middle(*args):
    outs = [local(XB, YB, ZB)] + [local(2, YB, ZB)] * 2 + [local(2, XB, ZB)] * 2
    return call(middle_kernel, outs, args, TOTAL, name="middle")


def last(*args):
    outs = [jax.ShapeDtypeStruct((2, XB, YB, ZB), jnp.float32)]
    return call(last_kernel, outs, args, TOTAL, name="last")[0]


PAIR_A = [(0, 1), (1, 0), (2, 3), (3, 2)]
PAIR_B = [(0, 3), (3, 0), (1, 2), (2, 1)]


def body(previous, feed_rate, kill_rate):
    sc = jnp.asarray(node_table(), jnp.float32)[lax.axis_index("node")]
    basis, sums = map(jnp.asarray, fourier())
    hold = lax.optimization_barrier
    x = previous[0]
    x0 = xs = (x[0], x[1])
    edges = (x[:, 0], x[:, XB - 1], x[:, :, 0], x[:, :, YB - 1])
    for sweep in range(SWEEPS):
        xfirst, xlast, yfirst, ylast = edges
        xlo = shifted(xlast, "sx", 1)
        xhi = shifted(xfirst, "sx", -1)
        ylo = shifted(ylast, "sy", 1)
        yhi = shifted(yfirst, "sy", -1)
        if sweep == 0:
            na = lax.ppermute(x[:, :HALF], "node", [(3, 2)])
            nb = lax.ppermute(x[:, HALF:], "node", [(3, 0)])
        fua, fub, fva, fvb, dua, dub, dva, dvb = forces(
            sc, *xs, xlo, xhi, ylo, yhi, feed_rate, kill_rate
        )
        fua, fub, na, nb = hold((fua, fub, na, nb))
        gua = lax.ppermute(fua, "node", PAIR_A)
        gub = lax.ppermute(fub, "node", PAIR_B)
        fva, fvb, gua, gub = hold((fva, fvb, gua, gub))
        gva = lax.ppermute(fva, "node", PAIR_A)
        gvb = lax.ppermute(fvb, "node", PAIR_B)
        done = []
        for s, (fa, fb, ga, gb, da, db) in enumerate(
            ((fua, fub, gua, gub, dua, dub), (fva, fvb, gva, gvb, dva, dvb))
        ):
            pa, pb = partial(s, sc, fa, fb, ga, gb, na, nb, x0[s])
            ra = lax.ppermute(pa, "node", PAIR_B)
            rb = lax.ppermute(pb, "node", PAIR_A)
            core, up, down = jacobi(
                s, sc, basis, sums, xs[s], x0[s], na, nb, fa, fb, ga, gb, da, db, ra, rb
            )
            low = shifted(up, "sy", 1)
            high = shifted(down, "sy", -1)
            left, right, center = gathered(sc, core, low, high)
            parts = (sc, basis, center, shifted(right, "sx", 1), shifted(left, "sx", -1))
            if s == 0:
                xu = first(*parts)
        if sweep + 1 < SWEEPS:
            xv, *edges = middle(*parts, xu)
            xs = (xu, xv)
    return last(*parts, xu)[None]


def solution(mesh):
    return jax.shard_map(
        body,
        mesh=mesh,
        in_specs=(P("node", None, "sx", "sy", None), P("sx", "sy", None), P("sx", "sy", None)),
        out_specs=P("node", None, "sx", "sy", None),
        check_vma=False,
    )
```

```python
import jax
import jax.numpy as jnp
import numpy as np
from jax import lax
from jax.experimental import pallas as pl
from jax.experimental.pallas import tpu as pltpu
from jax.sharding import PartitionSpec as P


SWEEPS = 2
JACOBI = 12


radau_points = [0.088587959512704, 0.409466864440735, 0.787659461760847, 1.0]
time_step = 4.0
diffusion_values = [1.0, 0.5]

XB, YB, ZB = 16, 32, 256
HALF = XB // 2
LANES = 128
PLANES = XB + 2 * (JACOBI + 1)
FIRST = JACOBI + 1
ROW0 = 24
ROWS = YB + 2 * ROW0
WHOLE = (FIRST - 4, XB + 8)


def shared_rows():
    pieces = []
    tile = WHOLE[1]
    for out in range(5, 12):
        pieces.append((tile, 0, FIRST - out, 1, JACOBI - out))
        pieces.append((tile, JACOBI - out, FIRST + XB - 1 + 16 - out, 1, out - 4))
        tile += 1
    thick = [FIRST + p for p in range(XB)]
    for left, right in zip(thick[::2], thick[1::2]):
        pieces.append((tile, 0, left, 9, 4))
        pieces.append((tile, 4, right, 9, 4))
        tile += 1
    for side in (lambda d: FIRST - d, lambda d: FIRST + XB - 1 + d):
        place = 0
        for out in range(1, 4):
            pieces.append((tile, place, side(out), 9, 4 - out))
            place += 4 - out
        tile += 1
    return pieces, tile


PIECES, STRIP = shared_rows()


def collocation():
    count = len(radau_points)
    table = []
    for _ in range(count):
        table.append([0.0] * count)
    for column in range(count):
        poly = [1.0]
        denom = 1.0
        for other in range(count):
            if other != column:
                longer = [0.0] * (len(poly) + 1)
                for place in range(len(poly)):
                    longer[place + 1] = longer[place + 1] + poly[place]
                    longer[place] = longer[place] - radau_points[other] * poly[place]
                poly = longer
                denom = denom * (radau_points[column] - radau_points[other])
        for row in range(count):
            point = radau_points[row]
            total = 0.0
            for place in range(len(poly)):
                total = total + poly[place] * point ** (place + 1) / (place + 1)
            table[row][column] = total / denom
    return table


def node_table():
    q = collocation()
    rows = []
    for n in range(4):
        a, b = n ^ 1, 3 - n
        common = [
            time_step * q[n][n], time_step * q[n][a], time_step * q[n][b],
            time_step * q[b][n], time_step * q[b][a],
            time_step * q[a][n], time_step * q[a][b],
            1.0 if n == 3 else 0.0,
        ]
        row = []
        for s, d in enumerate(diffusion_values):
            c = time_step * radau_points[n] * d
            row.append(common + [-c, c / (1.0 + 6.0 * c), 1.0 / (1.0 + 6.0 * c), d, float(s)])
        rows.append(row)
    return rows


def fourier():
    wave = np.arange(ZB)
    sine = wave > ZB // 2
    wave = np.where(sine, wave - ZB // 2, wave)
    norm = np.sqrt(np.where((wave == 0) | (wave == ZB // 2), 1.0, 2.0) / ZB)
    angle = 2.0 * np.pi * ((np.arange(0, ZB, 8)[:, None] * wave) % ZB) / ZB
    wide = norm * np.stack(
        [
            np.where(sine, np.sin(angle), np.cos(angle)),
            np.where(sine, np.cos(angle), -np.sin(angle)),
        ]
    )
    angle = 2.0 * np.pi * (np.arange(8)[:, None] * wave) / ZB
    near = np.stack([np.cos(angle), np.sin(angle)])
    sums = np.broadcast_to(2.0 * np.cos(2.0 * np.pi * wave / ZB), (8, ZB))
    return [v.astype(np.float32) for v in (wide, near, sums)]


def ring(count, step):
    return [(i, (i + step) % count) for i in range(count)]


def shifted(array, axis, step):
    return lax.ppermute(array, axis, ring(lax.axis_size(axis), step))


def call(kernel, outs, args, scratch=(), flops=1_000_000):
    vmem = pl.BlockSpec(memory_space=pltpu.VMEM)
    smem = pl.BlockSpec(memory_space=pltpu.SMEM)
    return pl.pallas_call(
        kernel,
        out_shape=tuple(outs),
        in_specs=[smem] + [vmem] * (len(args) - 1),
        out_specs=(vmem,) * len(outs),
        scratch_shapes=list(scratch),
        compiler_params=pltpu.CompilerParams(vmem_limit_bytes=24 * 2**20),
        cost_estimate=pl.CostEstimate(flops=flops, bytes_accessed=1_000_000, transcendentals=0),
    )(args[0], *(pltpu.with_memory_space_constraint(a, pltpu.VMEM) for a in args[1:]))


def local(*shape):
    return pltpu.VMEM(shape, jnp.float32)


def z_sum(c0, c1, lane):
    first, last = lane == 0, lane == LANES - 1
    up0, up1 = pltpu.roll(c0, 1, 1), pltpu.roll(c1, 1, 1)
    dn0, dn1 = pltpu.roll(c0, LANES - 1, 1), pltpu.roll(c1, LANES - 1, 1)
    low = jnp.where(first, up1, up0) + jnp.where(last, dn1, dn0)
    high = jnp.where(first, up0, up1) + jnp.where(last, dn0, dn1)
    return low, high


def force_kernel(species, sc, xu, xv, xlo, xhi, ylo, yhi, feed, kill, fa, fb, da, db, work):
    own = (xu, xv)[species]
    if len(xlo.shape) == 3:
        xlo, xhi, ylo, yhi = (edge.at[species] for edge in (xlo, xhi, ylo, yhi))

    def fill(p, carry):
        for h in range(2):
            lanes = slice(h * LANES, (h + 1) * LANES)
            work[p + 1, h, 8:8 + YB, :] = own[p, :, lanes]
        return carry

    lax.fori_loop(0, XB, fill, 0)
    for h in range(2):
        lanes = slice(h * LANES, (h + 1) * LANES)
        work[0, h, 8:8 + YB, :] = xlo[:, lanes]
        work[XB + 1, h, 8:8 + YB, :] = xhi[:, lanes]
        for p in range(XB):
            work[p + 1, h, 7:8, :] = ylo[p:p + 1, lanes]
            work[p + 1, h, 8 + YB:9 + YB, :] = yhi[p:p + 1, lanes]
    lane = lax.broadcasted_iota(jnp.int32, (8, LANES), 1)

    def run(base, f, d):
        def plane(i, carry):
            p = base + i
            for t in range(YB // 8):
                r = 8 + 8 * t
                out = slice(8 * t, 8 * t + 8)
                c = [work[p + 1, h, r:r + 8, :] for h in range(2)]
                z = z_sum(c[0], c[1], lane)
                for h in range(2):
                    lanes = slice(h * LANES, (h + 1) * LANES)
                    total = work[p, h, r:r + 8, :] + work[p + 2, h, r:r + 8, :]
                    total = total + work[p + 1, h, r - 1:r + 7, :]
                    total = total + work[p + 1, h, r + 1:r + 9, :]
                    lap = total + z[h] - 6.0 * c[h]
                    fr = feed[p, out, lanes]
                    u, v = xu[p, out, lanes], xv[p, out, lanes]
                    uvv = u * v * v
                    if species == 0:
                        react = fr * (1.0 - u) - uvv
                    else:
                        react = uvv - (fr + kill[p, out, lanes]) * v
                    f[i, out, lanes] = sc[11] * lap + react
                    d[i, out, lanes] = sc[8] * lap
            return carry

        lax.fori_loop(0, HALF, plane, 0)

    run(0, fa, da)
    run(HALF, fb, db)


def edges_of(x, xfirst, xlast, yfirst, ylast):
    xfirst[...] = x[0]
    xlast[...] = x[XB - 1]
    for p in range(XB):
        yfirst[p:p + 1, :] = x[p, 0:1, :]
        ylast[p:p + 1, :] = x[p, YB - 1:YB, :]


def prepare_kernel(sc, x, wide, near, xu, xv, ha, hb, basis, *edges):
    for a in range(ZB // 8):
        rows = wide[0, a:a + 1, :] * near[0] + wide[1, a:a + 1, :] * near[1]
        basis[8 * a:8 * a + 8, :] = rows
    for s, dst in enumerate((xu, xv)):
        edges_of(x.at[s], *(edge.at[s] for edge in edges))

        def plane(p, carry, s=s, dst=dst):
            dst[p] = x[s, p]
            dst[HALF + p] = x[s, HALF + p]
            ha[s, p] = x[s, p]
            hb[s, p] = x[s, HALF + p]
            return carry

        lax.fori_loop(0, HALF, plane, 0)


EDGES = [(YB, ZB)] * 2 + [(XB, ZB)] * 2


def prepare(*args):
    outs = [(XB, YB, ZB)] * 2 + [(2, HALF, YB, ZB)] * 2 + [(ZB, ZB)]
    outs += [(2, *e) for e in EDGES]
    return call(prepare_kernel, [local(*o) for o in outs], args)


def forces(species, *args):
    return call(
        lambda *refs: force_kernel(species, *refs),
        [local(HALF, YB, ZB)] * 4,
        args,
        [pltpu.VMEM((XB + 2, 2, YB + 16, LANES), jnp.float32)],
        flops=4_000_000,
    )


def partial_kernel(sc, fa, fb, ga, gb, na, nb, x0, sa, sb):
    species = sc[12].astype(jnp.int32)

    def plane(p, carry):
        low = na[species, p] + sc[7] * x0[p]
        high = nb[species, p] + sc[7] * x0[HALF + p]
        sa[p] = sc[3] * fa[p] + sc[4] * ga[p] + low
        sb[p] = sc[5] * fb[p] + sc[6] * gb[p] + high
        return carry

    lax.fori_loop(0, HALF, plane, 0)


def partial(*args):
    return call(partial_kernel, [local(HALF, YB, ZB)] * 2, args)


def jacobi_kernel(sc, basis, sums, x, x0, na, nb, fa, fb, ga, gb, da, db, ra, rb,
                  core, yhi, ylo, one, two, bs, right):
    spread, scale = sc[9], sc[10]
    species = sc[12].astype(jnp.int32)
    zero = jnp.zeros((ROWS, LANES), jnp.float32)

    def clear(p, carry):
        for h in range(2):
            one[p, h] = zero
            two[p, h] = zero
            bs[p, h] = zero[:YB]
        return carry

    lax.fori_loop(0, PLANES, clear, 0)

    def modes(values):
        flat = values.reshape(-1, ZB)
        done = jnp.dot(flat, basis[...], precision=lax.Precision.HIGHEST,
                       preferred_element_type=jnp.float32)
        return done.reshape(values.shape)

    def gather(half, f, g, d, n, recv, weight):
        def plane(i, carry):
            own = sc[0] * f[i] + sc[weight] * g[i] + d[i]
            own = own + (n[species, i] + sc[7] * x0[half * HALF + i])
            right[half * HALF + i] = own + recv[i]
            return carry

        lax.fori_loop(0, HALF, plane, 0)

    gather(0, fa, ga, da, na, ra, 1)
    gather(1, fb, gb, db, nb, rb, 2)

    def fill(i, carry):
        p = i * 4
        xh = modes(x[pl.ds(p, 4)])
        bh = modes(right[pl.ds(p, 4)])
        for h in range(2):
            lanes = slice(h * LANES, (h + 1) * LANES)
            one[pl.ds(FIRST + p, 4), h, ROW0:ROW0 + YB, :] = xh[:, :, lanes]
            bs[pl.ds(FIRST + p, 4), h] = scale * bh[:, :, lanes]
        return carry

    lax.fori_loop(0, XB // 4, fill, 0)
    turned = [spread * sums[:, h * LANES:(h + 1) * LANES] for h in range(2)]

    def one_plane(src, dst, p, group, carry):
        count = 2 * len(group)
        before, here = carry[:count], carry[count:]
        after = []
        for t in group:
            r = ROW0 + 8 * t
            after += [src[p + 1, h, r:r + 8, :] for h in range(2)]
        for j, t in enumerate(group):
            r = ROW0 + 8 * t
            for h in range(2):
                i = 2 * j + h
                total = before[i] + after[i]
                total = total + (src[p, h, r - 1:r + 7, :] + src[p, h, r + 1:r + 9, :])
                new = spread * total + turned[h] * here[i]
                if 0 <= t < YB // 8:
                    new = new + bs[p, h, 8 * t:8 * t + 8, :]
                dst[p, h, r:r + 8, :] = new
        return (*here, *after)

    def turn(src, dst, k, tiles):
        wide = (k + 1) // 2
        first = FIRST - 2 * wide
        span = list(range(-tiles, YB // 8 + tiles))
        for group in (span[:len(span) // 2], span[len(span) // 2:]):

            def step(i, carry, group=group):
                for j in range(4):
                    carry = one_plane(src, dst, first + 4 * i + j, group, carry)
                return carry

            carry = (jnp.zeros((8, LANES), jnp.float32),) * (4 * len(group))
            lax.fori_loop(0, XB // 4 + wide, step, carry)

    def pair(tiles):
        def run(i, carry):
            turn(one, two, 2 * i + 1, tiles)
            turn(two, one, 2 * i + 2, tiles)
            return carry

        return run

    lax.fori_loop(0, 4, pair(1), 0)
    lax.fori_loop(4, JACOBI // 2, pair(2), 0)

    def give(p, carry):
        for h in range(2):
            lanes = slice(h * LANES, (h + 1) * LANES)
            core[p, :, lanes] = one[p + 1, h, ROW0:ROW0 + YB, :]
        return carry

    lax.fori_loop(0, XB + 2 * JACOBI, give, 0)

    def whole(i, carry):
        for h in range(2):
            lanes = slice(h * LANES, (h + 1) * LANES)
            yhi[i, :, lanes] = one[WHOLE[0] + i, h, ROW0 + YB:ROW0 + YB + 8, :]
            ylo[i, :, lanes] = one[WHOLE[0] + i, h, ROW0 - 8:ROW0, :]
        return carry

    lax.fori_loop(0, WHOLE[1], whole, 0)
    for tile, place, p, row, count in PIECES:
        top, low = ROW0 + YB - 1 + row, ROW0 - row - count + 1
        for h in range(2):
            lanes = slice(h * LANES, (h + 1) * LANES)
            yhi[tile, place:place + count, lanes] = one[p, h, top:top + count, :]
            ylo[tile, place:place + count, lanes] = one[p, h, low:low + count, :]


def jacobi(*args):
    return call(
        jacobi_kernel,
        [local(XB + 2 * JACOBI, YB, ZB)] + [local(STRIP, 8, ZB)] * 2,
        args,
        [
            pltpu.VMEM((PLANES, 2, ROWS, LANES), jnp.float32),
            pltpu.VMEM((PLANES, 2, ROWS, LANES), jnp.float32),
            pltpu.VMEM((PLANES, 2, YB, LANES), jnp.float32),
            pltpu.VMEM((XB, YB, ZB), jnp.float32),
        ],
        flops=60_000_000,
    )


def gather_kernel(sc, core, low, high, xlo, xhi, center):
    def part(p):
        if p < JACOBI:
            return xlo, p
        if p < JACOBI + XB:
            return center, p - JACOBI
        return xhi, p - JACOBI - XB

    for p in range(XB + 2 * JACOBI):
        dst, q = part(p)
        whole = p + 1 - WHOLE[0]
        if 0 <= whole < WHOLE[1]:
            dst[q, :8, :] = core[p, :8, :] + low[whole]
            dst[q, 8:YB - 8, :] = core[p, 8:YB - 8, :]
            dst[q, YB - 8:, :] = core[p, YB - 8:, :] + high[whole]
        else:
            dst[q] = core[p]
    for tile, place, p, row, count in PIECES:
        dst, q = part(p - 1)
        end = YB - row + 1
        dst[q, row - 1:row - 1 + count, :] += low[tile, place:place + count, :]
        dst[q, end - count:end, :] += high[tile, place:place + count, :]


def gathered(*args):
    return call(gather_kernel, [local(JACOBI, YB, ZB)] * 2 + [local(XB, YB, ZB)], args)


def back(basis, c, low, high, total, give):
    gap = XB - JACOBI

    def add(p, carry):
        total[p] = c[p]
        return carry

    def add_low(p, carry):
        total[p] += low[p]
        return carry

    def add_high(p, carry):
        total[gap + p] += high[p]
        return carry

    lax.fori_loop(0, XB, add, 0)
    lax.fori_loop(0, JACOBI, add_low, 0)
    lax.fori_loop(0, JACOBI, add_high, 0)

    def turn(i, carry):
        flat = total[pl.ds(4 * i, 4)].reshape(4 * YB, ZB)
        done = lax.dot_general(flat, basis[...], (((1,), (1,)), ((), ())),
                               precision=lax.Precision.HIGHEST,
                               preferred_element_type=jnp.float32)
        give(4 * i, done.reshape(4, YB, ZB))
        return carry

    lax.fori_loop(0, XB // 4, turn, 0)


def middle_kernel(sc, basis, c, low, high, out, xfirst, xlast, yfirst, ylast, total):

    def give(p, value):
        out[pl.ds(p, 4)] = value

    back(basis, c, low, high, total, give)
    edges_of(out, xfirst, xlast, yfirst, ylast)


def last_kernel(sc, basis, c, low, high, xu, out, total):
    def give(p, value):
        out[1, pl.ds(p, 4)] = value

    def copy(p, carry):
        out[0, p] = xu[p]
        return carry

    lax.fori_loop(0, XB, copy, 0)
    back(basis, c, low, high, total, give)


TOTAL = [pltpu.VMEM((XB, YB, ZB), jnp.float32)]


def middle(*args):
    outs = [local(*o) for o in [(XB, YB, ZB)] + EDGES]
    return call(middle_kernel, outs, args, TOTAL)


def last(*args):
    outs = [jax.ShapeDtypeStruct((2, XB, YB, ZB), jnp.float32)]
    return call(last_kernel, outs, args, TOTAL)[0]


PAIR_A = [(0, 1), (1, 0), (2, 3), (3, 2)]
PAIR_B = [(0, 3), (3, 0), (1, 2), (2, 1)]


def body(previous, feed_rate, kill_rate):
    sc = jnp.asarray(node_table(), jnp.float32)[lax.axis_index("node")]
    wide, near, sums = map(jnp.asarray, fourier())
    hold = lax.optimization_barrier
    xu, xv, ha, hb, basis, *edges = prepare(sc[0], previous[0], wide, near)
    x0 = (xu, xv)
    na = lax.ppermute(ha, "node", [(3, 2)])
    nb = lax.ppermute(hb, "node", [(3, 0)])

    def halos_of(xfirst, xlast, yfirst, ylast):
        return (
            shifted(xlast, "sx", 1),
            shifted(xfirst, "sx", -1),
            shifted(ylast, "sy", 1),
            shifted(yfirst, "sy", -1),
        )

    for sweep in range(SWEEPS):
        more = sweep + 1 < SWEEPS
        xs = (xu, xv)
        if sweep == 0:
            halos = halos_of(*edges)
            fs = [forces(s, sc[s], *xs, *halos, feed_rate, kill_rate) for s in range(2)]
        else:
            fs = [forces(0, sc[0], *xs, *halos_of(*edges[0]), feed_rate, kill_rate)]
            *late, _, _ = hold((*edges[1], *fs[0][:2]))
            halos = halos_of(*late)
            fs.append(forces(1, sc[1], *xs, *halos, feed_rate, kill_rate))
        edges = []
        for s in range(2):
            fa, fb, da, db = fs[s]
            ga = lax.ppermute(fa, "node", PAIR_A)
            gb = lax.ppermute(fb, "node", PAIR_B)
            pa, pb = partial(sc[s], fa, fb, ga, gb, na, nb, x0[s])
            if s == 0:
                va, vb, _, _ = hold((*fs[1][:2], pa, pb))
                fs[1] = (va, vb, *fs[1][2:])
            ra = lax.ppermute(pa, "node", PAIR_B)
            rb = lax.ppermute(pb, "node", PAIR_A)
            if s == 1:
                ra, rb, _, _ = hold((ra, rb, left, right))
            core, up, down = jacobi(
                sc[s], basis, sums, xs[s], x0[s], na, nb, fa, fb, ga, gb, da, db, ra, rb
            )
            low = shifted(up, "sy", 1)
            high = shifted(down, "sy", -1)
            left, right, center = gathered(sc[0], core, low, high)
            low = shifted(right, "sx", 1)
            high = shifted(left, "sx", -1)
            parts = (sc[0], basis, center, low, high)
            if s == 0:
                xu, *rest = middle(*parts)
            elif more:
                xv, *rest = middle(*parts)
            edges.append(rest)
    return last(*parts, xu)[None]


def solution(mesh):
    return jax.shard_map(
        body,
        mesh=mesh,
        in_specs=(P("node", None, "sx", "sy", None), P("sx", "sy", None), P("sx", "sy", None)),
        out_specs=P("node", None, "sx", "sy", None),
        check_vma=False,
    )
```

```python
import jax
import jax.numpy as jnp
import numpy as np
from jax import lax
from jax.experimental import pallas as pl
from jax.experimental.pallas import tpu as pltpu
from jax.sharding import PartitionSpec as P


SWEEPS = 2
JACOBI = 12


radau_points = [0.088587959512704, 0.409466864440735, 0.787659461760847, 1.0]
time_step = 4.0
diffusion_values = [1.0, 0.5]

XB, YB, ZB = 16, 32, 256
HALF = XB // 2
LANES = 128
PLANES = XB + 2 * (JACOBI + 1)
FIRST = JACOBI + 1
ROW0 = 24
ROWS = YB + 2 * ROW0
WHOLE = (FIRST - 4, XB + 8)


def shared_rows():
    pieces = []
    tile = WHOLE[1]
    for out in range(5, 12):
        pieces.append((tile, 0, FIRST - out, 1, JACOBI - out))
        pieces.append((tile, JACOBI - out, FIRST + XB - 1 + 16 - out, 1, out - 4))
        tile += 1
    thick = [FIRST + p for p in range(XB)]
    for left, right in zip(thick[::2], thick[1::2]):
        pieces.append((tile, 0, left, 9, 4))
        pieces.append((tile, 4, right, 9, 4))
        tile += 1
    for side in (lambda d: FIRST - d, lambda d: FIRST + XB - 1 + d):
        place = 0
        for out in range(1, 4):
            pieces.append((tile, place, side(out), 9, 4 - out))
            place += 4 - out
        tile += 1
    return pieces, tile


PIECES, STRIP = shared_rows()


def collocation():
    count = len(radau_points)
    table = []
    for _ in range(count):
        table.append([0.0] * count)
    for column in range(count):
        poly = [1.0]
        denom = 1.0
        for other in range(count):
            if other != column:
                longer = [0.0] * (len(poly) + 1)
                for place in range(len(poly)):
                    longer[place + 1] = longer[place + 1] + poly[place]
                    longer[place] = longer[place] - radau_points[other] * poly[place]
                poly = longer
                denom = denom * (radau_points[column] - radau_points[other])
        for row in range(count):
            point = radau_points[row]
            total = 0.0
            for place in range(len(poly)):
                total = total + poly[place] * point ** (place + 1) / (place + 1)
            table[row][column] = total / denom
    return table


def node_table():
    q = collocation()
    rows = []
    for n in range(4):
        a, b = n ^ 1, 3 - n
        common = [
            time_step * q[n][n], time_step * q[n][a], time_step * q[n][b],
            time_step * q[b][n], time_step * q[b][a],
            time_step * q[a][n], time_step * q[a][b],
            1.0 if n == 3 else 0.0,
        ]
        row = []
        for s, d in enumerate(diffusion_values):
            c = time_step * radau_points[n] * d
            row.append(common + [-c, c / (1.0 + 6.0 * c), 1.0 / (1.0 + 6.0 * c), d, float(s)])
        rows.append(row)
    return rows


def fourier():
    wave = np.arange(ZB)
    sine = wave > ZB // 2
    wave = np.where(sine, wave - ZB // 2, wave)
    norm = np.sqrt(np.where((wave == 0) | (wave == ZB // 2), 1.0, 2.0) / ZB)
    angle = 2.0 * np.pi * ((np.arange(0, ZB, 8)[:, None] * wave) % ZB) / ZB
    wide = norm * np.stack(
        [
            np.where(sine, np.sin(angle), np.cos(angle)),
            np.where(sine, np.cos(angle), -np.sin(angle)),
        ]
    )
    angle = 2.0 * np.pi * (np.arange(8)[:, None] * wave) / ZB
    near = np.stack([np.cos(angle), np.sin(angle)])
    sums = np.broadcast_to(2.0 * np.cos(2.0 * np.pi * wave / ZB), (8, ZB))
    return [v.astype(np.float32) for v in (wide, near, sums)]


def ring(count, step):
    return [(i, (i + step) % count) for i in range(count)]


def shifted(array, axis, step):
    return lax.ppermute(array, axis, ring(lax.axis_size(axis), step))


def halves(values):
    high = values.astype(jnp.bfloat16)
    return high, (values - high.astype(jnp.float32)).astype(jnp.bfloat16)


def product(values, high, low, side):
    a, b = halves(values)

    def dot(x, y):
        return lax.dot_general(x, y[...], (((1,), (side,)), ((), ())),
                               preferred_element_type=jnp.float32)

    return dot(a, high) + (dot(a, low) + dot(b, high))


def call(kernel, outs, args, scratch=(), flops=1_000_000):
    vmem = pl.BlockSpec(memory_space=pltpu.VMEM)
    smem = pl.BlockSpec(memory_space=pltpu.SMEM)
    return pl.pallas_call(
        kernel,
        out_shape=tuple(outs),
        in_specs=[smem] + [vmem] * (len(args) - 1),
        out_specs=(vmem,) * len(outs),
        scratch_shapes=list(scratch),
        compiler_params=pltpu.CompilerParams(vmem_limit_bytes=24 * 2**20),
        cost_estimate=pl.CostEstimate(flops=flops, bytes_accessed=1_000_000, transcendentals=0),
    )(args[0], *(pltpu.with_memory_space_constraint(a, pltpu.VMEM) for a in args[1:]))


def local(*shape):
    return pltpu.VMEM(shape, jnp.float32)


def z_sum(c0, c1, lane):
    first, last = lane == 0, lane == LANES - 1
    up0, up1 = pltpu.roll(c0, 1, 1), pltpu.roll(c1, 1, 1)
    dn0, dn1 = pltpu.roll(c0, LANES - 1, 1), pltpu.roll(c1, LANES - 1, 1)
    low = jnp.where(first, up1, up0) + jnp.where(last, dn1, dn0)
    high = jnp.where(first, up0, up1) + jnp.where(last, dn0, dn1)
    return low, high


def force_kernel(species, sc, xu, xv, xlo, xhi, ylo, yhi, feed, kill, fa, fb, da, db, work):
    own = (xu, xv)[species]
    if len(xlo.shape) == 3:
        xlo, xhi, ylo, yhi = (edge.at[species] for edge in (xlo, xhi, ylo, yhi))

    def fill(p, carry):
        for h in range(2):
            lanes = slice(h * LANES, (h + 1) * LANES)
            work[p + 1, h, 8:8 + YB, :] = own[p, :, lanes]
        return carry

    lax.fori_loop(0, XB, fill, 0)
    for h in range(2):
        lanes = slice(h * LANES, (h + 1) * LANES)
        work[0, h, 8:8 + YB, :] = xlo[:, lanes]
        work[XB + 1, h, 8:8 + YB, :] = xhi[:, lanes]
        for p in range(XB):
            work[p + 1, h, 7:8, :] = ylo[p:p + 1, lanes]
            work[p + 1, h, 8 + YB:9 + YB, :] = yhi[p:p + 1, lanes]
    lane = lax.broadcasted_iota(jnp.int32, (8, LANES), 1)

    def run(base, f, d):
        def plane(i):
            p = base + i
            for t in range(YB // 8):
                r = 8 + 8 * t
                out = slice(8 * t, 8 * t + 8)
                c = [work[p + 1, h, r:r + 8, :] for h in range(2)]
                z = z_sum(c[0], c[1], lane)
                for h in range(2):
                    lanes = slice(h * LANES, (h + 1) * LANES)
                    total = work[p, h, r:r + 8, :] + work[p + 2, h, r:r + 8, :]
                    total = total + work[p + 1, h, r - 1:r + 7, :]
                    total = total + work[p + 1, h, r + 1:r + 9, :]
                    lap = total + z[h] - 6.0 * c[h]
                    fr = feed[p, out, lanes]
                    u, v = xu[p, out, lanes], xv[p, out, lanes]
                    uvv = u * v * v
                    if species == 0:
                        react = fr * (1.0 - u) - uvv
                    else:
                        react = uvv - (fr + kill[p, out, lanes]) * v
                    f[i, out, lanes] = sc[11] * lap + react
                    d[i, out, lanes] = sc[8] * lap

        def planes(i, carry):
            plane(2 * i)
            plane(2 * i + 1)
            return carry

        lax.fori_loop(0, HALF // 2, planes, 0)

    run(0, fa, da)
    run(HALF, fb, db)


def edges_of(x, xfirst, xlast, yfirst, ylast):
    xfirst[...] = x[0]
    xlast[...] = x[XB - 1]
    for p in range(XB):
        yfirst[p:p + 1, :] = x[p, 0:1, :]
        ylast[p:p + 1, :] = x[p, YB - 1:YB, :]


def prepare_kernel(sc, x, wide, near, xu, xv, ha, hb, bhi, blo, *edges):
    for a in range(0, ZB // 8, 2):
        rows = jnp.concatenate(
            [wide[0, b:b + 1, :] * near[0] + wide[1, b:b + 1, :] * near[1] for b in (a, a + 1)], 0
        )
        bhi[8 * a:8 * a + 16, :], blo[8 * a:8 * a + 16, :] = halves(rows)
    for s, dst in enumerate((xu, xv)):
        edges_of(x.at[s], *(edge.at[s] for edge in edges))

        def plane(p, carry, s=s, dst=dst):
            dst[p] = x[s, p]
            dst[HALF + p] = x[s, HALF + p]
            ha[s, p] = x[s, p]
            hb[s, p] = x[s, HALF + p]
            return carry

        lax.fori_loop(0, HALF, plane, 0)


EDGES = [(YB, ZB)] * 2 + [(XB, ZB)] * 2


def prepare(*args):
    outs = [local(*o) for o in [(XB, YB, ZB)] * 2 + [(2, HALF, YB, ZB)] * 2]
    outs += [pltpu.VMEM((ZB, ZB), jnp.bfloat16)] * 2 + [local(2, *e) for e in EDGES]
    return call(prepare_kernel, outs, args)


def forces(species, *args):
    return call(
        lambda *refs: force_kernel(species, *refs),
        [local(HALF, YB, ZB)] * 4,
        args,
        [pltpu.VMEM((XB + 2, 2, YB + 16, LANES), jnp.float32)],
        flops=4_000_000,
    )


def partial_kernel(sc, fa, fb, ga, gb, na, nb, x0, sa, sb):
    species = sc[12].astype(jnp.int32)

    def plane(p, carry):
        low = na[species, p] + sc[7] * x0[p]
        high = nb[species, p] + sc[7] * x0[HALF + p]
        sa[p] = sc[3] * fa[p] + sc[4] * ga[p] + low
        sb[p] = sc[5] * fb[p] + sc[6] * gb[p] + high
        return carry

    lax.fori_loop(0, HALF, plane, 0)


def partial(*args):
    return call(partial_kernel, [local(HALF, YB, ZB)] * 2, args)


def jacobi_kernel(sc, bhi, blo, sums, x, x0, na, nb, fa, fb, ga, gb, da, db, ra, rb,
                  core, yhi, ylo, one, two, bs, right):
    spread, scale = sc[9], sc[10]
    species = sc[12].astype(jnp.int32)
    zero = jnp.zeros((ROWS, LANES), jnp.float32)

    def clear(p, carry):
        for h in range(2):
            one[p, h] = zero
            two[p, h] = zero
            bs[p, h] = zero[:YB]
        return carry

    lax.fori_loop(0, PLANES, clear, 0)

    def modes(values):
        return product(values.reshape(-1, ZB), bhi, blo, 0).reshape(values.shape)

    def gather(half, f, g, d, n, recv, weight):
        def plane(i, carry):
            own = sc[0] * f[i] + sc[weight] * g[i] + d[i]
            own = own + (n[species, i] + sc[7] * x0[half * HALF + i])
            right[half * HALF + i] = own + recv[i]
            return carry

        lax.fori_loop(0, HALF, plane, 0)

    gather(0, fa, ga, da, na, ra, 1)
    gather(1, fb, gb, db, nb, rb, 2)

    def fill(i, carry):
        p = i * 4
        xh = modes(x[pl.ds(p, 4)])
        bh = modes(right[pl.ds(p, 4)])
        for h in range(2):
            lanes = slice(h * LANES, (h + 1) * LANES)
            one[pl.ds(FIRST + p, 4), h, ROW0:ROW0 + YB, :] = xh[:, :, lanes]
            bs[pl.ds(FIRST + p, 4), h] = scale * bh[:, :, lanes]
        return carry

    lax.fori_loop(0, XB // 4, fill, 0)
    turned = [spread * sums[:, h * LANES:(h + 1) * LANES] for h in range(2)]

    def one_plane(src, dst, p, group, carry):
        count = 2 * len(group)
        before, here = carry[:count], carry[count:]
        after = []
        for t in group:
            r = ROW0 + 8 * t
            after += [src[p + 1, h, r:r + 8, :] for h in range(2)]
        for j, t in enumerate(group):
            r = ROW0 + 8 * t
            for h in range(2):
                i = 2 * j + h
                total = before[i] + after[i]
                total = total + (src[p, h, r - 1:r + 7, :] + src[p, h, r + 1:r + 9, :])
                new = spread * total + turned[h] * here[i]
                if 0 <= t < YB // 8:
                    new = new + bs[p, h, 8 * t:8 * t + 8, :]
                dst[p, h, r:r + 8, :] = new
        return (*here, *after)

    def turn(src, dst, k, tiles):
        wide = (k + 1) // 2
        first = FIRST - 2 * wide
        span = list(range(-tiles, YB // 8 + tiles))
        for group in (span[:len(span) // 2], span[len(span) // 2:]):

            def step(i, carry, group=group):
                for j in range(4):
                    carry = one_plane(src, dst, first + 4 * i + j, group, carry)
                return carry

            carry = (jnp.zeros((8, LANES), jnp.float32),) * (4 * len(group))
            lax.fori_loop(0, XB // 4 + wide, step, carry)

    def pair(tiles):
        def run(i, carry):
            turn(one, two, 2 * i + 1, tiles)
            turn(two, one, 2 * i + 2, tiles)
            return carry

        return run

    lax.fori_loop(0, 4, pair(1), 0)
    lax.fori_loop(4, JACOBI // 2, pair(2), 0)

    def give(p, carry):
        for h in range(2):
            lanes = slice(h * LANES, (h + 1) * LANES)
            core[p, :, lanes] = one[p + 1, h, ROW0:ROW0 + YB, :]
        return carry

    lax.fori_loop(0, XB + 2 * JACOBI, give, 0)

    def whole(i, carry):
        for h in range(2):
            lanes = slice(h * LANES, (h + 1) * LANES)
            yhi[i, :, lanes] = one[WHOLE[0] + i, h, ROW0 + YB:ROW0 + YB + 8, :]
            ylo[i, :, lanes] = one[WHOLE[0] + i, h, ROW0 - 8:ROW0, :]
        return carry

    lax.fori_loop(0, WHOLE[1], whole, 0)
    for tile, place, p, row, count in PIECES:
        top, low = ROW0 + YB - 1 + row, ROW0 - row - count + 1
        for h in range(2):
            lanes = slice(h * LANES, (h + 1) * LANES)
            yhi[tile, place:place + count, lanes] = one[p, h, top:top + count, :]
            ylo[tile, place:place + count, lanes] = one[p, h, low:low + count, :]


def jacobi(*args):
    return call(
        jacobi_kernel,
        [local(XB + 2 * JACOBI, YB, ZB)] + [local(STRIP, 8, ZB)] * 2,
        args,
        [
            pltpu.VMEM((PLANES, 2, ROWS, LANES), jnp.float32),
            pltpu.VMEM((PLANES, 2, ROWS, LANES), jnp.float32),
            pltpu.VMEM((PLANES, 2, YB, LANES), jnp.float32),
            pltpu.VMEM((XB, YB, ZB), jnp.float32),
        ],
        flops=60_000_000,
    )


def gather_kernel(sc, core, low, high, xlo, xhi, center):
    def part(p):
        if p < JACOBI:
            return xlo, p
        if p < JACOBI + XB:
            return center, p - JACOBI
        return xhi, p - JACOBI - XB

    for p in range(XB + 2 * JACOBI):
        dst, q = part(p)
        whole = p + 1 - WHOLE[0]
        if 0 <= whole < WHOLE[1]:
            dst[q, :8, :] = core[p, :8, :] + low[whole]
            dst[q, 8:YB - 8, :] = core[p, 8:YB - 8, :]
            dst[q, YB - 8:, :] = core[p, YB - 8:, :] + high[whole]
        else:
            dst[q] = core[p]
    for tile, place, p, row, count in PIECES:
        dst, q = part(p - 1)
        end = YB - row + 1
        dst[q, row - 1:row - 1 + count, :] += low[tile, place:place + count, :]
        dst[q, end - count:end, :] += high[tile, place:place + count, :]


def gathered(*args):
    return call(gather_kernel, [local(JACOBI, YB, ZB)] * 2 + [local(XB, YB, ZB)], args)


def back(bhi, blo, c, low, high, total, give):
    gap = XB - JACOBI

    def add(p, carry):
        total[p] = c[p]
        return carry

    def add_low(p, carry):
        total[p] += low[p]
        return carry

    def add_high(p, carry):
        total[gap + p] += high[p]
        return carry

    lax.fori_loop(0, XB, add, 0)
    lax.fori_loop(0, JACOBI, add_low, 0)
    lax.fori_loop(0, JACOBI, add_high, 0)

    def turn(i, carry):
        flat = total[pl.ds(8 * i, 8)].reshape(8 * YB, ZB)
        done = product(flat, bhi, blo, 1)
        give(8 * i, done.reshape(8, YB, ZB))
        return carry

    lax.fori_loop(0, XB // 8, turn, 0)


def middle_kernel(sc, bhi, blo, c, low, high, out, xfirst, xlast, yfirst, ylast, total):

    def give(p, value):
        out[pl.ds(p, 8)] = value

    back(bhi, blo, c, low, high, total, give)
    edges_of(out, xfirst, xlast, yfirst, ylast)


def last_kernel(sc, bhi, blo, c, low, high, xu, out, total):
    def give(p, value):
        out[1, pl.ds(p, 8)] = value

    def copy(p, carry):
        out[0, p] = xu[p]
        return carry

    lax.fori_loop(0, XB, copy, 0)
    back(bhi, blo, c, low, high, total, give)


TOTAL = [pltpu.VMEM((XB, YB, ZB), jnp.float32)]


def middle(*args):
    outs = [local(*o) for o in [(XB, YB, ZB)] + EDGES]
    return call(middle_kernel, outs, args, TOTAL)


def last(*args):
    outs = [jax.ShapeDtypeStruct((2, XB, YB, ZB), jnp.float32)]
    return call(last_kernel, outs, args, TOTAL)[0]


PAIR_A = [(0, 1), (1, 0), (2, 3), (3, 2)]
PAIR_B = [(0, 3), (3, 0), (1, 2), (2, 1)]


def body(previous, feed_rate, kill_rate):
    sc = jnp.asarray(node_table(), jnp.float32)[lax.axis_index("node")]
    wide, near, sums = map(jnp.asarray, fourier())
    hold = lax.optimization_barrier
    xu, xv, ha, hb, bhi, blo, *edges = prepare(sc[0], previous[0], wide, near)
    x0 = (xu, xv)
    na = lax.ppermute(ha, "node", [(3, 2)])
    nb = lax.ppermute(hb, "node", [(3, 0)])

    def halos_of(xfirst, xlast, yfirst, ylast):
        return (
            shifted(xlast, "sx", 1),
            shifted(xfirst, "sx", -1),
            shifted(ylast, "sy", 1),
            shifted(yfirst, "sy", -1),
        )

    for sweep in range(SWEEPS):
        more = sweep + 1 < SWEEPS
        xs = (xu, xv)
        if sweep == 0:
            halos = halos_of(*edges)
            fs = [forces(s, sc[s], *xs, *halos, feed_rate, kill_rate) for s in range(2)]
        else:
            fs = [forces(0, sc[0], *xs, *halos_of(*edges[0]), feed_rate, kill_rate)]
            *late, _, _ = hold((*edges[1], *fs[0][:2]))
            halos = halos_of(*late)
            fs.append(forces(1, sc[1], *xs, *halos, feed_rate, kill_rate))
        edges = []
        for s in range(2):
            fa, fb, da, db = fs[s]
            ga = lax.ppermute(fa, "node", PAIR_A)
            gb = lax.ppermute(fb, "node", PAIR_B)
            pa, pb = partial(sc[s], fa, fb, ga, gb, na, nb, x0[s])
            if s == 0:
                va, vb, _, _ = hold((*fs[1][:2], pa, pb))
                fs[1] = (va, vb, *fs[1][2:])
            ra = lax.ppermute(pa, "node", PAIR_B)
            rb = lax.ppermute(pb, "node", PAIR_A)
            if s == 1:
                ra, rb, _, _ = hold((ra, rb, left, right))
            core, up, down = jacobi(
                sc[s], bhi, blo, sums, xs[s], x0[s], na, nb, fa, fb, ga, gb, da, db, ra, rb
            )
            low = shifted(up, "sy", 1)
            high = shifted(down, "sy", -1)
            left, right, center = gathered(sc[0], core, low, high)
            low = shifted(right, "sx", 1)
            high = shifted(left, "sx", -1)
            parts = (sc[0], bhi, blo, center, low, high)
            if s == 0:
                xu, *rest = middle(*parts)
            elif more:
                xv, *rest = middle(*parts)
            edges.append(rest)
    return last(*parts, xu)[None]


def solution(mesh):
    return jax.shard_map(
        body,
        mesh=mesh,
        in_specs=(P("node", None, "sx", "sy", None), P("sx", "sy", None), P("sx", "sy", None)),
        out_specs=P("node", None, "sx", "sy", None),
        check_vma=False,
    )
```

```python
import jax
import jax.numpy as jnp
import numpy as np
from jax import lax
from jax.experimental import pallas as pl
from jax.experimental.pallas import tpu as pltpu
from jax.sharding import PartitionSpec as P


SWEEPS = 2
JACOBI = 12


radau_points = [0.088587959512704, 0.409466864440735, 0.787659461760847, 1.0]
time_step = 4.0
diffusion_values = [1.0, 0.5]

XB, YB, ZB = 16, 32, 256
HALF = XB // 2
LANES = 128
PLANES = XB + 2 * (JACOBI + 1)
FIRST = JACOBI + 1
ROW0 = 24
ROWS = YB + 2 * ROW0
WHOLE = (FIRST - 4, XB + 8)


def shared_rows():
    pieces = []
    tile = WHOLE[1]
    for out in range(5, 12):
        pieces.append((tile, 0, FIRST - out, 1, JACOBI - out))
        pieces.append((tile, JACOBI - out, FIRST + XB - 1 + 16 - out, 1, out - 4))
        tile += 1
    thick = [FIRST + p for p in range(XB)]
    for left, right in zip(thick[::2], thick[1::2]):
        pieces.append((tile, 0, left, 9, 4))
        pieces.append((tile, 4, right, 9, 4))
        tile += 1
    for side in (lambda d: FIRST - d, lambda d: FIRST + XB - 1 + d):
        place = 0
        for out in range(1, 4):
            pieces.append((tile, place, side(out), 9, 4 - out))
            place += 4 - out
        tile += 1
    return pieces, tile


PIECES, STRIP = shared_rows()


def collocation():
    count = len(radau_points)
    table = []
    for _ in range(count):
        table.append([0.0] * count)
    for column in range(count):
        poly = [1.0]
        denom = 1.0
        for other in range(count):
            if other != column:
                longer = [0.0] * (len(poly) + 1)
                for place in range(len(poly)):
                    longer[place + 1] = longer[place + 1] + poly[place]
                    longer[place] = longer[place] - radau_points[other] * poly[place]
                poly = longer
                denom = denom * (radau_points[column] - radau_points[other])
        for row in range(count):
            point = radau_points[row]
            total = 0.0
            for place in range(len(poly)):
                total = total + poly[place] * point ** (place + 1) / (place + 1)
            table[row][column] = total / denom
    return table


def node_table():
    q = collocation()
    rows = []
    for n in range(4):
        a, b = n ^ 1, 3 - n
        common = [
            time_step * q[n][n], time_step * q[n][a], time_step * q[n][b],
            time_step * q[b][n], time_step * q[b][a],
            time_step * q[a][n], time_step * q[a][b],
            1.0 if n == 3 else 0.0,
        ]
        row = []
        for s, d in enumerate(diffusion_values):
            c = time_step * radau_points[n] * d
            row.append(common + [-c, c / (1.0 + 6.0 * c), 1.0 / (1.0 + 6.0 * c), d, float(s)])
        rows.append(row)
    return rows


def fourier():
    wave = np.arange(ZB)
    sine = wave > ZB // 2
    wave = np.where(sine, wave - ZB // 2, wave)
    norm = np.sqrt(np.where((wave == 0) | (wave == ZB // 2), 1.0, 2.0) / ZB)
    angle = 2.0 * np.pi * ((np.arange(0, ZB, 8)[:, None] * wave) % ZB) / ZB
    wide = norm * np.stack(
        [
            np.where(sine, np.sin(angle), np.cos(angle)),
            np.where(sine, np.cos(angle), -np.sin(angle)),
        ]
    )
    angle = 2.0 * np.pi * (np.arange(8)[:, None] * wave) / ZB
    near = np.stack([np.cos(angle), np.sin(angle)])
    sums = np.broadcast_to(2.0 * np.cos(2.0 * np.pi * wave / ZB), (8, ZB))
    return [v.astype(np.float32) for v in (wide, near, sums)]


def ring(count, step):
    return [(i, (i + step) % count) for i in range(count)]


def shifted(array, axis, step):
    return lax.ppermute(array, axis, ring(lax.axis_size(axis), step))


def halves(values):
    high = values.astype(jnp.bfloat16)
    return high, (values - high.astype(jnp.float32)).astype(jnp.bfloat16)


def product(values, high, low, side):
    a, b = halves(values)

    def dot(x, y):
        return lax.dot_general(x, y[...], (((1,), (side,)), ((), ())),
                               preferred_element_type=jnp.float32)

    return dot(a, high) + (dot(a, low) + dot(b, high))


def call(kernel, outs, args, scratch=(), flops=1_000_000):
    vmem = pl.BlockSpec(memory_space=pltpu.VMEM)
    smem = pl.BlockSpec(memory_space=pltpu.SMEM)
    return pl.pallas_call(
        kernel,
        out_shape=tuple(outs),
        in_specs=[smem] + [vmem] * (len(args) - 1),
        out_specs=(vmem,) * len(outs),
        scratch_shapes=list(scratch),
        compiler_params=pltpu.CompilerParams(vmem_limit_bytes=24 * 2**20),
        cost_estimate=pl.CostEstimate(flops=flops, bytes_accessed=1_000_000, transcendentals=0),
    )(args[0], *(pltpu.with_memory_space_constraint(a, pltpu.VMEM) for a in args[1:]))


def local(*shape):
    return pltpu.VMEM(shape, jnp.float32)


def z_sum(c0, c1, lane):
    first, last = lane == 0, lane == LANES - 1
    up0, up1 = pltpu.roll(c0, 1, 1), pltpu.roll(c1, 1, 1)
    dn0, dn1 = pltpu.roll(c0, LANES - 1, 1), pltpu.roll(c1, LANES - 1, 1)
    low = jnp.where(first, up1, up0) + jnp.where(last, dn1, dn0)
    high = jnp.where(first, up0, up1) + jnp.where(last, dn0, dn1)
    return low, high


def force_kernel(species, sc, xu, xv, xlo, xhi, ylo, yhi, feed, kill, fa, fb, da, db, work):
    own = (xu, xv)[species]
    if len(xlo.shape) == 3:
        xlo, xhi, ylo, yhi = (edge.at[species] for edge in (xlo, xhi, ylo, yhi))

    def fill(p, carry):
        for h in range(2):
            lanes = slice(h * LANES, (h + 1) * LANES)
            work[p + 1, h, 8:8 + YB, :] = own[p, :, lanes]
        return carry

    lax.fori_loop(0, XB, fill, 0)
    for h in range(2):
        lanes = slice(h * LANES, (h + 1) * LANES)
        work[0, h, 8:8 + YB, :] = xlo[:, lanes]
        work[XB + 1, h, 8:8 + YB, :] = xhi[:, lanes]
        for p in range(XB):
            work[p + 1, h, 7:8, :] = ylo[p:p + 1, lanes]
            work[p + 1, h, 8 + YB:9 + YB, :] = yhi[p:p + 1, lanes]
    lane = lax.broadcasted_iota(jnp.int32, (8, LANES), 1)

    def run(base, f, d):
        def plane(i):
            p = base + i
            for t in range(YB // 8):
                r = 8 + 8 * t
                out = slice(8 * t, 8 * t + 8)
                c = [work[p + 1, h, r:r + 8, :] for h in range(2)]
                z = z_sum(c[0], c[1], lane)
                for h in range(2):
                    lanes = slice(h * LANES, (h + 1) * LANES)
                    total = work[p, h, r:r + 8, :] + work[p + 2, h, r:r + 8, :]
                    total = total + work[p + 1, h, r - 1:r + 7, :]
                    total = total + work[p + 1, h, r + 1:r + 9, :]
                    lap = total + z[h] - 6.0 * c[h]
                    fr = feed[p, out, lanes]
                    u, v = xu[p, out, lanes], xv[p, out, lanes]
                    uvv = u * v * v
                    if species == 0:
                        react = fr * (1.0 - u) - uvv
                    else:
                        react = uvv - (fr + kill[p, out, lanes]) * v
                    f[i, out, lanes] = sc[11] * lap + react
                    d[i, out, lanes] = sc[8] * lap

        def planes(i, carry):
            plane(2 * i)
            plane(2 * i + 1)
            return carry

        lax.fori_loop(0, HALF // 2, planes, 0)

    run(0, fa, da)
    run(HALF, fb, db)


def edges_of(x, xfirst, xlast, yfirst, ylast):
    xfirst[...] = x[0]
    xlast[...] = x[XB - 1]
    for p in range(XB):
        yfirst[p:p + 1, :] = x[p, 0:1, :]
        ylast[p:p + 1, :] = x[p, YB - 1:YB, :]


def prepare_kernel(sc, x, wide, near, xu, xv, hua, hub, hva, hvb, bhi, blo, *edges):
    for a in range(0, ZB // 8, 2):
        rows = jnp.concatenate(
            [wide[0, b:b + 1, :] * near[0] + wide[1, b:b + 1, :] * near[1] for b in (a, a + 1)], 0
        )
        bhi[8 * a:8 * a + 16, :], blo[8 * a:8 * a + 16, :] = halves(rows)
    for s, (dst, ha, hb) in enumerate(((xu, hua, hub), (xv, hva, hvb))):
        edges_of(x.at[s], *(edge.at[s] for edge in edges))

        def plane(p, carry, s=s, dst=dst, ha=ha, hb=hb):
            dst[p] = x[s, p]
            dst[HALF + p] = x[s, HALF + p]
            ha[p] = x[s, p]
            hb[p] = x[s, HALF + p]
            return carry

        lax.fori_loop(0, HALF, plane, 0)


EDGES = [(YB, ZB)] * 2 + [(XB, ZB)] * 2


def prepare(*args):
    outs = [local(*o) for o in [(XB, YB, ZB)] * 2 + [(HALF, YB, ZB)] * 4]
    outs += [pltpu.VMEM((ZB, ZB), jnp.bfloat16)] * 2 + [local(2, *e) for e in EDGES]
    return call(prepare_kernel, outs, args)


def forces(species, *args):
    return call(
        lambda *refs: force_kernel(species, *refs),
        [local(HALF, YB, ZB)] * 4,
        args,
        [pltpu.VMEM((XB + 2, 2, YB + 16, LANES), jnp.float32)],
        flops=4_000_000,
    )


def partial_kernel(sc, fa, fb, ga, gb, na, nb, x0, sa, sb):
    def plane(p, carry):
        low = na[p] + sc[7] * x0[p]
        high = nb[p] + sc[7] * x0[HALF + p]
        sa[p] = sc[3] * fa[p] + sc[4] * ga[p] + low
        sb[p] = sc[5] * fb[p] + sc[6] * gb[p] + high
        return carry

    lax.fori_loop(0, HALF, plane, 0)


def partial(*args):
    return call(partial_kernel, [local(HALF, YB, ZB)] * 2, args)


def jacobi_kernel(sc, bhi, blo, sums, x, x0, na, nb, fa, fb, ga, gb, da, db, ra, rb,
                  core, yhi, ylo, one, two, bs, right):
    spread, scale = sc[9], sc[10]
    zero = jnp.zeros((ROWS, LANES), jnp.float32)

    def clear(p, carry):
        for h in range(2):
            one[p, h] = zero
            two[p, h] = zero
            bs[p, h] = zero[:YB]
        return carry

    lax.fori_loop(0, PLANES, clear, 0)

    def modes(values):
        return product(values.reshape(-1, ZB), bhi, blo, 0).reshape(values.shape)

    def gather(half, f, g, d, n, recv, weight):
        def plane(i, carry):
            own = sc[0] * f[i] + sc[weight] * g[i] + d[i]
            own = own + (n[i] + sc[7] * x0[half * HALF + i])
            right[half * HALF + i] = own + recv[i]
            return carry

        lax.fori_loop(0, HALF, plane, 0)

    gather(0, fa, ga, da, na, ra, 1)
    gather(1, fb, gb, db, nb, rb, 2)

    def fill(i, carry):
        p = i * 4
        xh = modes(x[pl.ds(p, 4)])
        bh = modes(right[pl.ds(p, 4)])
        for h in range(2):
            lanes = slice(h * LANES, (h + 1) * LANES)
            one[pl.ds(FIRST + p, 4), h, ROW0:ROW0 + YB, :] = xh[:, :, lanes]
            bs[pl.ds(FIRST + p, 4), h] = scale * bh[:, :, lanes]
        return carry

    lax.fori_loop(0, XB // 4, fill, 0)
    turned = [spread * sums[:, h * LANES:(h + 1) * LANES] for h in range(2)]

    def one_plane(src, dst, p, group, carry):
        count = 2 * len(group)
        before, here = carry[:count], carry[count:]
        after = []
        for t in group:
            r = ROW0 + 8 * t
            after += [src[p + 1, h, r:r + 8, :] for h in range(2)]
        for j, t in enumerate(group):
            r = ROW0 + 8 * t
            for h in range(2):
                i = 2 * j + h
                total = before[i] + after[i]
                total = total + (src[p, h, r - 1:r + 7, :] + src[p, h, r + 1:r + 9, :])
                new = spread * total + turned[h] * here[i]
                if 0 <= t < YB // 8:
                    new = new + bs[p, h, 8 * t:8 * t + 8, :]
                dst[p, h, r:r + 8, :] = new
        return (*here, *after)

    def turn(src, dst, k, tiles):
        wide = (k + 1) // 2
        first = FIRST - 2 * wide
        span = list(range(-tiles, YB // 8 + tiles))
        for group in (span[:len(span) // 2], span[len(span) // 2:]):

            def step(i, carry, group=group):
                for j in range(4):
                    carry = one_plane(src, dst, first + 4 * i + j, group, carry)
                return carry

            carry = (jnp.zeros((8, LANES), jnp.float32),) * (4 * len(group))
            lax.fori_loop(0, XB // 4 + wide, step, carry)

    def pair(tiles):
        def run(i, carry):
            turn(one, two, 2 * i + 1, tiles)
            turn(two, one, 2 * i + 2, tiles)
            return carry

        return run

    lax.fori_loop(0, 4, pair(1), 0)
    lax.fori_loop(4, JACOBI // 2, pair(2), 0)

    def give(p, carry):
        for h in range(2):
            lanes = slice(h * LANES, (h + 1) * LANES)
            core[p, :, lanes] = one[p + 1, h, ROW0:ROW0 + YB, :]
        return carry

    lax.fori_loop(0, XB + 2 * JACOBI, give, 0)

    def whole(i, carry):
        for h in range(2):
            lanes = slice(h * LANES, (h + 1) * LANES)
            yhi[i, :, lanes] = one[WHOLE[0] + i, h, ROW0 + YB:ROW0 + YB + 8, :]
            ylo[i, :, lanes] = one[WHOLE[0] + i, h, ROW0 - 8:ROW0, :]
        return carry

    lax.fori_loop(0, WHOLE[1], whole, 0)
    for tile, place, p, row, count in PIECES:
        top, low = ROW0 + YB - 1 + row, ROW0 - row - count + 1
        for h in range(2):
            lanes = slice(h * LANES, (h + 1) * LANES)
            yhi[tile, place:place + count, lanes] = one[p, h, top:top + count, :]
            ylo[tile, place:place + count, lanes] = one[p, h, low:low + count, :]


def jacobi(*args):
    return call(
        jacobi_kernel,
        [local(XB + 2 * JACOBI, YB, ZB)] + [local(STRIP, 8, ZB)] * 2,
        args,
        [
            pltpu.VMEM((PLANES, 2, ROWS, LANES), jnp.float32),
            pltpu.VMEM((PLANES, 2, ROWS, LANES), jnp.float32),
            pltpu.VMEM((PLANES, 2, YB, LANES), jnp.float32),
            pltpu.VMEM((XB, YB, ZB), jnp.float32),
        ],
        flops=60_000_000,
    )


def gather_kernel(sc, core, low, high, xlo, xhi, center):
    def part(p):
        if p < JACOBI:
            return xlo, p
        if p < JACOBI + XB:
            return center, p - JACOBI
        return xhi, p - JACOBI - XB

    for p in range(XB + 2 * JACOBI):
        dst, q = part(p)
        whole = p + 1 - WHOLE[0]
        if 0 <= whole < WHOLE[1]:
            dst[q, :8, :] = core[p, :8, :] + low[whole]
            dst[q, 8:YB - 8, :] = core[p, 8:YB - 8, :]
            dst[q, YB - 8:, :] = core[p, YB - 8:, :] + high[whole]
        else:
            dst[q] = core[p]
    for tile, place, p, row, count in PIECES:
        dst, q = part(p - 1)
        end = YB - row + 1
        dst[q, row - 1:row - 1 + count, :] += low[tile, place:place + count, :]
        dst[q, end - count:end, :] += high[tile, place:place + count, :]


def gathered(*args):
    return call(gather_kernel, [local(JACOBI, YB, ZB)] * 2 + [local(XB, YB, ZB)], args)


def back(bhi, blo, c, low, high, total, give):
    gap = XB - JACOBI

    def add(p, carry):
        total[p] = c[p]
        return carry

    def add_low(p, carry):
        total[p] += low[p]
        return carry

    def add_high(p, carry):
        total[gap + p] += high[p]
        return carry

    lax.fori_loop(0, XB, add, 0)
    lax.fori_loop(0, JACOBI, add_low, 0)
    lax.fori_loop(0, JACOBI, add_high, 0)

    def turn(i, carry):
        flat = total[pl.ds(8 * i, 8)].reshape(8 * YB, ZB)
        done = product(flat, bhi, blo, 1)
        give(8 * i, done.reshape(8, YB, ZB))
        return carry

    lax.fori_loop(0, XB // 8, turn, 0)


def middle_kernel(sc, bhi, blo, c, low, high, out, xfirst, xlast, yfirst, ylast, total):

    def give(p, value):
        out[pl.ds(p, 8)] = value

    back(bhi, blo, c, low, high, total, give)
    edges_of(out, xfirst, xlast, yfirst, ylast)


def last_kernel(sc, bhi, blo, c, low, high, xu, out, total):
    def give(p, value):
        out[1, pl.ds(p, 8)] = value

    def copy(p, carry):
        out[0, p] = xu[p]
        return carry

    lax.fori_loop(0, XB, copy, 0)
    back(bhi, blo, c, low, high, total, give)


TOTAL = [pltpu.VMEM((XB, YB, ZB), jnp.float32)]


def middle(*args):
    outs = [local(*o) for o in [(XB, YB, ZB)] + EDGES]
    return call(middle_kernel, outs, args, TOTAL)


def last(*args):
    outs = [jax.ShapeDtypeStruct((2, XB, YB, ZB), jnp.float32)]
    return call(last_kernel, outs, args, TOTAL)[0]


PAIR_A = [(0, 1), (1, 0), (2, 3), (3, 2)]
PAIR_B = [(0, 3), (3, 0), (1, 2), (2, 1)]


def body(previous, feed_rate, kill_rate):
    sc = jnp.asarray(node_table(), jnp.float32)[lax.axis_index("node")]
    wide, near, sums = map(jnp.asarray, fourier())
    hold = lax.optimization_barrier
    xu, xv, hua, hub, hva, hvb, bhi, blo, *edges = prepare(sc[0], previous[0], wide, near)
    x0 = (xu, xv)

    def start(a, b):
        return lax.ppermute(a, "node", [(3, 2)]), lax.ppermute(b, "node", [(3, 0)])

    starts = [start(hua, hub)]

    def halos_of(xfirst, xlast, yfirst, ylast):
        return (
            shifted(xlast, "sx", 1),
            shifted(xfirst, "sx", -1),
            shifted(ylast, "sy", 1),
            shifted(yfirst, "sy", -1),
        )

    for sweep in range(SWEEPS):
        more = sweep + 1 < SWEEPS
        xs = (xu, xv)
        if sweep == 0:
            halos = halos_of(*edges)
            fs = [forces(s, sc[s], *xs, *halos, feed_rate, kill_rate) for s in range(2)]
        else:
            fs = [forces(0, sc[0], *xs, *halos_of(*edges[0]), feed_rate, kill_rate)]
            *late, _, _ = hold((*edges[1], *fs[0][:2]))
            halos = halos_of(*late)
            fs.append(forces(1, sc[1], *xs, *halos, feed_rate, kill_rate))
        edges = []
        for s in range(2):
            fa, fb, da, db = fs[s]
            ga = lax.ppermute(fa, "node", PAIR_A)
            gb = lax.ppermute(fb, "node", PAIR_B)
            if s == len(starts):
                hva, hvb, _, _ = hold((hva, hvb, pa, pb))
                starts.append(start(hva, hvb))
            na, nb = starts[s]
            pa, pb = partial(sc[s], fa, fb, ga, gb, na, nb, x0[s])
            if s == 0:
                va, vb, _, _ = hold((*fs[1][:2], pa, pb))
                fs[1] = (va, vb, *fs[1][2:])
            ra = lax.ppermute(pa, "node", PAIR_B)
            rb = lax.ppermute(pb, "node", PAIR_A)
            if s == 1:
                ra, rb, _, _ = hold((ra, rb, left, right))
            core, up, down = jacobi(
                sc[s], bhi, blo, sums, xs[s], x0[s], na, nb, fa, fb, ga, gb, da, db, ra, rb
            )
            low = shifted(up, "sy", 1)
            high = shifted(down, "sy", -1)
            left, right, center = gathered(sc[0], core, low, high)
            low = shifted(right, "sx", 1)
            high = shifted(left, "sx", -1)
            parts = (sc[0], bhi, blo, center, low, high)
            if s == 0:
                xu, *rest = middle(*parts)
            elif more:
                xv, *rest = middle(*parts)
            edges.append(rest)
    return last(*parts, xu)[None]


def solution(mesh):
    return jax.shard_map(
        body,
        mesh=mesh,
        in_specs=(P("node", None, "sx", "sy", None), P("sx", "sy", None), P("sx", "sy", None)),
        out_specs=P("node", None, "sx", "sy", None),
        check_vma=False,
    )
```
